32 devices in a mesh: samp: 8 (over z, x), win: 1, snp: 4 (over y, core).
Axes of the slice: x: 2, y: 2, z: 4, core: 2. Of those that a mesh axis runs over, the one named last changes fastest.
Arguments:
- dosages: bfloat16 [4096, 4096], P('samp', ('win', 'snp')), may hold values from 0 to 2
Outputs:
- r_squared: float32 [1, 4096, 4096], P('win', 'samp', 'snp')
- band_r_squared: float32 [1, 1024, 4096], P('win', 'samp', 'snp')
The draws below stay inside these ranges and needn't reach their ends.
All inputs are finite; a program needn't handle non-finite values.
Results may differ from the reference program's by a relative error of at most 0.0003.
Values may be sent and summed in bfloat16 or wider, within the bound.
A program may use at most 128 MiB of HBM per device.

```python
import jax
import jax.numpy as jnp
from jax import lax

WS = 4096
OV = 1024
WINDOWS = 1
SAMPLES = 4096
SNPS = 4096


def draw_dosages(key, part):
    keys = jax.random.split(key, 5)
    span = min(24, SNPS)
    noise = jax.random.normal(keys[0], (SAMPLES, SNPS), jnp.float32)
    smooth = lax.reduce_window(noise, 0.0, lax.add, (1, span), (1, 1), 'SAME') / span ** 0.5
    own_weight = jax.random.uniform(keys[1], (SNPS,), jnp.float32, 0.3, 1.0)
    mix_weight = jax.random.uniform(keys[2], (SNPS,), jnp.float32, 0.5, 2.5)
    people = jax.random.normal(keys[3], (SAMPLES, 1), jnp.float32)
    loading = jax.random.normal(keys[4], (SNPS,), jnp.float32) * 0.6
    latent = noise * own_weight + smooth * mix_weight
    latent = latent + people * loading
    return (2.0 * jax.nn.sigmoid(latent)).astype(jnp.bfloat16)


def setup_inputs(seed: int = 0) -> dict:
    seeds = jax.random.split(jax.random.key(seed), 2)
    return {
        "dosages": draw_dosages(jax.random.fold_in(seeds[1], 71), 0),
    }


var_floor = 0.05


def squared_corr(gram, col_sum, col_sq, row_sum, row_sq, count):
    col_mean = col_sum / count
    row_mean = row_sum / count
    col_var = jnp.maximum(col_sq / count - col_mean * col_mean, var_floor)
    row_var = jnp.maximum(row_sq / count - row_mean * row_mean, var_floor)
    covar = gram / count - col_mean[:, None] * row_mean[None, :]
    return covar * covar / (col_var[:, None] * row_var[None, :])


def column_stats(block):
    wide = block.astype(jnp.float32)
    return jnp.sum(wide, axis=0), jnp.sum(wide * wide, axis=0)


def reference(dosages):
    count = jnp.float32(dosages.shape[0])
    whole_list = []
    band_list = []
    for window in range(WINDOWS):
        geno = dosages[:, window * WS:(window + 1) * WS]
        following = (window + 1) % WINDOWS
        after = dosages[:, following * WS:following * WS + OV]
        win_sum, win_sq = column_stats(geno)
        next_sum, next_sq = column_stats(after)
        gram = jnp.dot(geno.T, geno, preferred_element_type=jnp.float32)
        next_gram = jnp.dot(after.T, geno, preferred_element_type=jnp.float32)
        whole_list.append(squared_corr(gram, win_sum, win_sq, win_sum, win_sq, count))
        band_list.append(squared_corr(next_gram, next_sum, next_sq, win_sum, win_sq, count))
    return jnp.stack(whole_list), jnp.stack(band_list)
```

```python
import functools
import heapq

import jax
import jax.numpy as jnp
from jax import lax
from jax.experimental import pallas as pl
from jax.experimental.pallas import tpu as pltpu
from jax.sharding import PartitionSpec as P

OV = 1024
VAR_FLOOR = 0.05
COLS = 2
PARTS = 4
LATE = PARTS // 2
MESH = pl.DeviceIdType.MESH


def by_z(z, zz, c):
    return c >= LATE and abs(z - zz) == 1


def sends(line, z, item):
    side, zz, c = item
    out = []
    if side == 0:
        if zz <= z and z < line - 1:
            out.append((1, item))
        if zz >= z and z > 0:
            out.append((-1, item))
        if not by_z(z, zz, c):
            out.append((0, item))
        if c == PARTS - 1:
            for way, far in ((-1, line - 1), (1, 0)):
                if zz == far and 0 <= z + way < line and last_on(line, z, way):
                    out += [(way, (1, z, k)) for k in range(LATE, PARTS)]
    elif zz == z and c >= LATE:
        for way in (-1, 1):
            if 0 <= z + way < line and not last_on(line, z, way):
                out.append((way, item))
    return out


def last_on(line, z, way):
    return z < line // 2 if way < 0 else z >= line // 2


def plan(line):
    hop = 1.0
    lag = 0.35
    events = [(0.0, z * PARTS + c, z, (0, z, c)) for z in range(line) for c in range(PARTS)]
    heapq.heapify(events)
    free = {}
    order = [[] for _ in range(line)]
    count = line * PARTS
    while events:
        t, _, z, item = heapq.heappop(events)
        order[z].append(item)
        for way, (side, zz, c) in sends(line, z, item):
            begin = max(free.get((z, way), 0.0), t)
            free[z, way] = begin + hop
            moved = (side, zz, c) if way else (1 - side, zz, c)
            heapq.heappush(events, (begin + hop + lag, count, z + way, moved))
            count += 1
    for z in range(line // 2, line):
        order[z] = [(side, line - 1 - zz, c) for side, zz, c in order[line - 1 - z]]
    return order


def lookup(i, values):
    out = jnp.int32(0)
    for j, v in enumerate(values):
        if v:
            out = out + jnp.where(i == j, jnp.int32(v), jnp.int32(0))
    return out


def kernel(sizes, x_hbm, win_out, band_out, k_buf, j_buf, b_buf, k_stat, j_stat, b_stat,
           local_sem, k_recv, up_send, down_send, x_send, j_recv, j_send, b_recv, b_send, w_send, *band_wide):
    shard_count, windows, blocks, rows, width, jw, band, bw = sizes
    line = shard_count // COLS
    part_rows = rows // PARTS
    bits = blocks.bit_length() - 1
    chunks = shard_count * PARTS
    s = lax.axis_index("samp")
    n = lax.axis_index("snp")
    z = s // COLS
    x = s % COLS
    has_up = z < line - 1
    has_down = z > 0
    up = {"samp": jnp.minimum(s + COLS, shard_count - COLS + x)}
    down = {"samp": jnp.maximum(s - COLS, x)}
    across = {"samp": s + 1 - 2 * x}

    def bit(v, b):
        return (v // (1 << b)) % 2

    def flip(b):
        return {"snp": n + (1 << b) * (1 - 2 * bit(n, b))}

    j_home = (s * jw) // width
    j_off = pl.multiple_of((s * jw) % width, jw)
    b_home = (s * band) // width
    b_off = pl.multiple_of(((s * band) % width) // bw * bw, bw)
    j_rel = [(bit(n, b) + bit(j_home, b)) % 2 for b in range(bits)]
    b_rel = [(bit(n, b) + bit(b_home, b)) % 2 for b in range(bits)]

    def sends_on(rel, b):
        low = jnp.int32(0)
        for a in range(b + 1):
            low = low + rel[a]
        return low == 0

    def is_home(rel):
        total = jnp.int32(0)
        for r in rel:
            total = total + r
        return total == 0

    j_mine = is_home(j_rel)
    b_mine = is_home(b_rel)

    def k_copy(q, sem, to):
        return pltpu.make_async_remote_copy(
            src_ref=k_buf.at[q], dst_ref=k_buf.at[q], send_sem=sem.at[q], recv_sem=k_recv.at[q],
            device_id=to, device_id_type=MESH)

    def slice_copy(src, buf, q, send, recv, to):
        return pltpu.make_async_remote_copy(
            src_ref=src, dst_ref=buf.at[q], send_sem=send, recv_sem=recv.at[q],
            device_id=to, device_id_type=MESH)

    order = plan(line)
    band_sum = band_wide[0] if band_wide else band_out
    low = z < line // 2
    near_z = jnp.where(low, z, line - 1 - z)

    def item(o):
        code = jnp.int32(0)
        for half in range((line + 1) // 2):
            mine = lookup(o, [(side * line + zz) * PARTS + c for side, zz, c in order[half]])
            code = code + jnp.where(near_z == half, mine, 0)
        c = code % PARTS
        zz = (code // PARTS) % line
        side = code // (PARTS * line)
        zz = jnp.where(low, zz, line - 1 - zz)
        xx = jnp.where(side == 1, 1 - x, x)
        return side, zz, c, (zz * COLS + xx) * PARTS + c

    def skips_x(zz, c):
        return (c >= LATE) & ((zz == z + 1) | (zz == z - 1))

    crossed = [(s + 1 - 2 * x) * PARTS + c for c in range(LATE, PARTS)]
    up_last = has_up & (z >= line // 2)
    down_last = has_down & (z < line // 2)
    up_soon = has_up & (z < line // 2)
    down_soon = has_down & (z >= line // 2)

    for c in range(PARTS):
        pltpu.make_async_copy(x_hbm.at[pl.ds(c * part_rows, part_rows)],
                              k_buf.at[s * PARTS + c], local_sem.at[c]).start()

    barrier = pltpu.get_barrier_semaphore()

    def greet(to):
        pl.semaphore_signal(barrier, inc=1, device_id=to, device_id_type=MESH)

    pl.when(has_up)(lambda: greet(up))
    pl.when(has_down)(lambda: greet(down))
    greet(across)
    for b in range(bits):
        greet(flip(b))
    expected = 1 + bits
    if windows > 1:
        w = lax.axis_index("win")
        before = {"win": (w + windows - 1) % windows}
        after = {"win": (w + 1) % windows}
        greet(before)
        greet(after)
        expected += 2
    pl.semaphore_wait(barrier, expected + has_up.astype(jnp.int32) + has_down.astype(jnp.int32))

    k_stat[...] = jnp.zeros_like(k_stat)
    j_stat[...] = jnp.zeros_like(j_stat)
    b_stat[...] = jnp.zeros_like(b_stat)
    win_out[...] = jnp.zeros_like(win_out)
    band_sum[...] = jnp.zeros_like(band_sum)

    def take(o):
        side, zz, c, q = item(o)
        mine = (side == 0) & (zz == z)

        @pl.when(mine)
        def _():
            pltpu.make_async_copy(x_hbm.at[pl.ds(c * part_rows, part_rows)],
                                  k_buf.at[s * PARTS + c], local_sem.at[c]).wait()

        @pl.when(jnp.logical_not(mine))
        def _():
            k_copy(q, x_send, across).wait_recv()

        @pl.when((side == 0) & (zz <= z) & has_up)
        def _():
            k_copy(q, up_send, up).start()

        @pl.when((side == 0) & (zz >= z) & has_down)
        def _():
            k_copy(q, down_send, down).start()

        @pl.when((side == 0) & jnp.logical_not(skips_x(zz, c)))
        def _():
            k_copy(q, x_send, across).start()

        if line > 1:
            passes = (side == 1) & (zz == z) & (c >= LATE)
            ends = (side == 0) & (c == PARTS - 1)

            @pl.when(passes & up_soon)
            def _():
                k_copy(q, up_send, up).start()

            @pl.when(passes & down_soon)
            def _():
                k_copy(q, down_send, down).start()

            @pl.when(ends & (zz == 0) & up_last)
            def _():
                for k in crossed:
                    k_copy(k, up_send, up).start()

            @pl.when(ends & (zz == line - 1) & down_last)
            def _():
                for k in crossed:
                    k_copy(k, down_send, down).start()

        for b in reversed(range(bits)):
            @pl.when(j_mine)
            def _():
                slice_copy(k_buf.at[q, :, pl.ds(j_off, jw)], j_buf, q, j_send.at[b, q], j_recv, flip(b)).start()

            if windows == 1:
                @pl.when(b_mine)
                def _():
                    slice_copy(k_buf.at[q, :, pl.ds(b_off, bw)], b_buf, q, b_send.at[b, q], b_recv, flip(b)).start()
        if windows > 1:
            @pl.when(b_mine)
            def _():
                slice_copy(k_buf.at[q, :, pl.ds(b_off, bw)], b_buf, q, w_send.at[q], b_recv, before).start()

    def j_arrive(q):
        slice_copy(k_buf.at[q, :, pl.ds(j_off, jw)], j_buf, q, j_send.at[0, q], j_recv, flip(0)).wait_recv()

    def b_arrive(q):
        slice_copy(k_buf.at[q, :, pl.ds(b_off, bw)], b_buf, q, b_send.at[0, q], b_recv, flip(0)).wait_recv()

    def relay(o):
        _, _, _, q = item(o)

        @pl.when(jnp.logical_not(j_mine))
        def _():
            j_arrive(q)
            for b in reversed(range(bits)):
                @pl.when(sends_on(j_rel, b))
                def _():
                    slice_copy(j_buf.at[q], j_buf, q, j_send.at[b, q], j_recv, flip(b)).start()

        @pl.when(j_mine)
        def _():
            j_buf[q] = k_buf[q, :, pl.ds(j_off, jw)]

        def pass_band():
            b_arrive(q)
            for b in reversed(range(bits)):
                @pl.when(sends_on(b_rel, b))
                def _():
                    slice_copy(b_buf.at[q], b_buf, q, b_send.at[b, q], b_recv, flip(b)).start()

        if windows > 1:
            pass_band()
        else:
            pl.when(jnp.logical_not(b_mine))(pass_band)

            @pl.when(b_mine)
            def _():
                b_buf[q] = k_buf[q, :, pl.ds(b_off, bw)]

    def add_stats(stat, block):
        wide = block.astype(jnp.float32).reshape(part_rows // 8, 8, block.shape[-1])
        stat[0] += jnp.sum(wide, axis=0)
        stat[1] += jnp.sum(wide * wide, axis=0)

    def pair(a, b):
        return lax.dot_general(a, b, (((0,), (0,)), ((), ())), preferred_element_type=jnp.float32)

    def compute(o):
        _, _, _, q = item(o)
        whole = k_buf[q]
        j_cols = j_buf[q]
        b_cols = b_buf[q]
        add_stats(k_stat, whole)
        add_stats(j_stat, j_cols)
        add_stats(b_stat, b_cols)

        win_out[0] += pair(j_cols, whole)
        band_sum[0] += pair(b_cols, whole)

    def step(o, carry):
        @pl.when(o < chunks)
        def _():
            take(o)

        @pl.when((o >= 2) & (o < chunks + 2))
        def _():
            relay(o - 2)

        @pl.when(o >= 3)
        def _():
            compute(o - 3)

        return carry

    lax.fori_loop(0, chunks + 3, step, 0)

    count = jnp.float32(rows * shard_count)

    def moments(total, square):
        mean = total / count
        return mean, 1.0 / jnp.maximum(square / count - mean * mean, VAR_FLOOR)

    row_mean, row_inv = moments(jnp.sum(k_stat[0], axis=0, keepdims=True), jnp.sum(k_stat[1], axis=0, keepdims=True))

    def finish(out, stat, height):
        mean, inv = moments(jnp.sum(stat[0].T, axis=1, keepdims=True), jnp.sum(stat[1].T, axis=1, keepdims=True))
        for a in range(0, height, 64):
            e = min(a + 64, height)
            covar = out[0, a:e] / count - mean[a:e] * row_mean
            out[0, a:e] = covar * covar * (inv[a:e] * row_inv)

    finish(win_out, j_stat, jw)
    finish(band_sum, b_stat, bw)
    if band_wide:
        band_out[0] = band_sum[0, pl.ds(pl.multiple_of((s * band) % bw, band), band)]

    def drain(o, carry):
        side, zz, c, q = item(o)

        @pl.when((side == 0) & (zz <= z) & has_up)
        def _():
            k_copy(q, up_send, up).wait_send()

        @pl.when((side == 0) & (zz >= z) & has_down)
        def _():
            k_copy(q, down_send, down).wait_send()

        @pl.when((side == 0) & jnp.logical_not(skips_x(zz, c)))
        def _():
            k_copy(q, x_send, across).wait_send()

        for b in range(bits):
            @pl.when(sends_on(j_rel, b))
            def _():
                slice_copy(j_buf.at[q], j_buf, q, j_send.at[b, q], j_recv, flip(b)).wait_send()

            @pl.when(sends_on(b_rel, b))
            def _():
                slice_copy(b_buf.at[q], b_buf, q, b_send.at[b, q], b_recv, flip(b)).wait_send()
        if windows > 1:
            @pl.when(b_mine)
            def _():
                slice_copy(b_buf.at[q], b_buf, q, w_send.at[q], b_recv, before).wait_send()
        return carry

    lax.fori_loop(0, chunks, drain, 0)
    if line > 1:
        for k in crossed:
            @pl.when(has_up)
            def _():
                k_copy(k, up_send, up).wait_send()

            @pl.when(has_down)
            def _():
                k_copy(k, down_send, down).wait_send()


def shards(dosages):
    rows, width = dosages.shape
    shard_count = lax.axis_size("samp")
    windows = lax.axis_size("win")
    blocks = lax.axis_size("snp")
    jw = width * blocks // shard_count
    band = OV // shard_count
    bw = max(band, 128)
    bits = blocks.bit_length() - 1
    chunks = shard_count * PARTS
    part_rows = rows // PARTS
    sizes = (shard_count, windows, blocks, rows, width, jw, band, bw)
    dma = pltpu.SemaphoreType.DMA
    return pl.pallas_call(
        functools.partial(kernel, sizes),
        out_shape=(
            jax.ShapeDtypeStruct((1, jw, width), jnp.float32),
            jax.ShapeDtypeStruct((1, band, width), jnp.float32),
        ),
        in_specs=[pl.BlockSpec(memory_space=pl.ANY)],
        out_specs=[pl.BlockSpec(memory_space=pltpu.VMEM)] * 2,
        scratch_shapes=[
            pltpu.VMEM((chunks, part_rows, width), jnp.bfloat16),
            pltpu.VMEM((chunks, part_rows, jw), jnp.bfloat16),
            pltpu.VMEM((chunks, part_rows, bw), jnp.bfloat16),
            pltpu.VMEM((2, 8, width), jnp.float32),
            pltpu.VMEM((2, 8, jw), jnp.float32),
            pltpu.VMEM((2, 8, bw), jnp.float32),
            dma((PARTS,)),
            dma((chunks,)), dma((chunks,)), dma((chunks,)), dma((chunks,)),
            dma((chunks,)), dma((bits, chunks)),
            dma((chunks,)), dma((bits, chunks)), dma((chunks,)),
        ] + ([pltpu.VMEM((1, bw, width), jnp.float32)] if bw != band else []),
        compiler_params=pltpu.CompilerParams(
            collective_id=0, has_side_effects=True, vmem_limit_bytes=67043328
        ),
    )(dosages)


def solution(mesh):
    return jax.shard_map(
        shards,
        mesh=mesh,
        in_specs=(P("samp", ("win", "snp")),),
        out_specs=(P("win", "samp", "snp"), P("win", "samp", "snp")),
        check_vma=False,
    )
```

```python
import functools
import heapq

import jax
import jax.numpy as jnp
from jax import lax
from jax.experimental import pallas as pl
from jax.experimental.pallas import tpu as pltpu
from jax.sharding import PartitionSpec as P

OV = 1024
VAR_FLOOR = 0.05
COLS = 2
PARTS = 4
LATE = PARTS // 2
PASS = 2
USE = 4
MESH = pl.DeviceIdType.MESH


def by_z(z, zz, c):
    return c >= LATE and abs(z - zz) == 1


def sends(line, z, item):
    side, zz, c = item
    out = []
    if side == 0:
        if zz <= z and z < line - 1:
            out.append((1, item))
        if zz >= z and z > 0:
            out.append((-1, item))
        if not by_z(z, zz, c):
            out.append((0, item))
        if c == PARTS - 1:
            for way, far in ((-1, line - 1), (1, 0)):
                if zz == far and 0 <= z + way < line and last_on(line, z, way):
                    out += [(way, (1, z, k)) for k in range(LATE, PARTS)]
    elif zz == z and c >= LATE:
        for way in (-1, 1):
            if 0 <= z + way < line and not last_on(line, z, way):
                out.append((way, item))
    return out


def last_on(line, z, way):
    return z < line // 2 if way < 0 else z >= line // 2


def plan(line):
    hop = 1.0
    lag = 0.35
    events = [(0.0, z * PARTS + c, z, (0, z, c)) for z in range(line) for c in range(PARTS)]
    heapq.heapify(events)
    free = {}
    order = [[] for _ in range(line)]
    count = line * PARTS
    while events:
        t, _, z, item = heapq.heappop(events)
        order[z].append(item)
        for way, (side, zz, c) in sends(line, z, item):
            begin = max(free.get((z, way), 0.0), t)
            free[z, way] = begin + hop
            moved = (side, zz, c) if way else (1 - side, zz, c)
            heapq.heappush(events, (begin + hop + lag, count, z + way, moved))
            count += 1
    for z in range(line // 2, line):
        order[z] = [(side, line - 1 - zz, c) for side, zz, c in order[line - 1 - z]]
    return order


def lookup(i, values):
    out = jnp.int32(0)
    for j, v in enumerate(values):
        if v:
            out = out + jnp.where(i == j, jnp.int32(v), jnp.int32(0))
    return out


def kernel(sizes, x_hbm, win_out, band_out, k_buf, j_buf, b_buf, k_stat, j_stat, b_stat,
           local_sem, k_recv, up_send, down_send, x_send, j_recv, j_send, b_recv, b_send, w_send, *band_wide):
    shard_count, windows, blocks, rows, width, jw, band, bw = sizes
    line = shard_count // COLS
    part_rows = rows // PARTS
    bits = blocks.bit_length() - 1
    chunks = shard_count * PARTS
    s = lax.axis_index("samp")
    n = lax.axis_index("snp")
    z = s // COLS
    x = s % COLS
    has_up = z < line - 1
    has_down = z > 0
    up = {"samp": jnp.minimum(s + COLS, shard_count - COLS + x)}
    down = {"samp": jnp.maximum(s - COLS, x)}
    across = {"samp": s + 1 - 2 * x}

    def bit(v, b):
        return (v // (1 << b)) % 2

    def flip(b):
        return {"snp": n + (1 << b) * (1 - 2 * bit(n, b))}

    j_home = (s * jw) // width
    j_off = pl.multiple_of((s * jw) % width, jw)
    b_home = (s * band) // width
    b_off = pl.multiple_of(((s * band) % width) // bw * bw, bw)
    j_rel = [(bit(n, b) + bit(j_home, b)) % 2 for b in range(bits)]
    b_rel = [(bit(n, b) + bit(b_home, b)) % 2 for b in range(bits)]

    def sends_on(rel, b):
        low = jnp.int32(0)
        for a in range(b + 1):
            low = low + rel[a]
        return low == 0

    def is_home(rel):
        total = jnp.int32(0)
        for r in rel:
            total = total + r
        return total == 0

    j_mine = is_home(j_rel)
    b_mine = is_home(b_rel)

    def k_copy(q, sem, to):
        return pltpu.make_async_remote_copy(
            src_ref=k_buf.at[q], dst_ref=k_buf.at[q], send_sem=sem, recv_sem=k_recv.at[q],
            device_id=to, device_id_type=MESH)

    def slice_copy(src, buf, q, send, recv, to):
        return pltpu.make_async_remote_copy(
            src_ref=src, dst_ref=buf.at[q], send_sem=send, recv_sem=recv.at[q],
            device_id=to, device_id_type=MESH)

    order = plan(line)
    band_sum = band_wide[0] if band_wide else band_out
    low = z < line // 2
    near_z = jnp.where(low, z, line - 1 - z)

    def item(o):
        code = jnp.int32(0)
        for half in range((line + 1) // 2):
            mine = lookup(o, [(side * line + zz) * PARTS + c for side, zz, c in order[half]])
            code = code + jnp.where(near_z == half, mine, 0)
        c = code % PARTS
        zz = (code // PARTS) % line
        side = code // (PARTS * line)
        zz = jnp.where(low, zz, line - 1 - zz)
        xx = jnp.where(side == 1, 1 - x, x)
        return side, zz, c, (zz * COLS + xx) * PARTS + c

    def skips_x(zz, c):
        return (c >= LATE) & ((zz == z + 1) | (zz == z - 1))

    crossed = [(s + 1 - 2 * x) * PARTS + c for c in range(LATE, PARTS)]
    up_last = has_up & (z >= line // 2)
    down_last = has_down & (z < line // 2)
    up_soon = has_up & (z < line // 2)
    down_soon = has_down & (z >= line // 2)

    for c in range(PARTS):
        pltpu.make_async_copy(x_hbm.at[pl.ds(c * part_rows, part_rows)],
                              k_buf.at[s * PARTS + c], local_sem.at[c]).start()

    barrier = pltpu.get_barrier_semaphore()

    def greet(to):
        pl.semaphore_signal(barrier, inc=1, device_id=to, device_id_type=MESH)

    pl.when(has_up)(lambda: greet(up))
    pl.when(has_down)(lambda: greet(down))
    greet(across)
    for b in range(bits):
        greet(flip(b))
    expected = 1 + bits
    if windows > 1:
        w = lax.axis_index("win")
        before = {"win": (w + windows - 1) % windows}
        after = {"win": (w + 1) % windows}
        greet(before)
        greet(after)
        expected += 2
    pl.semaphore_wait(barrier, expected + has_up.astype(jnp.int32) + has_down.astype(jnp.int32))

    k_stat[...] = jnp.zeros_like(k_stat)
    j_stat[...] = jnp.zeros_like(j_stat)
    b_stat[...] = jnp.zeros_like(b_stat)
    win_out[...] = jnp.zeros_like(win_out)
    band_sum[...] = jnp.zeros_like(band_sum)

    def take(side, zz, c, q):
        mine = (side == 0) & (zz == z)

        @pl.when(mine)
        def _():
            pltpu.make_async_copy(x_hbm.at[pl.ds(c * part_rows, part_rows)],
                                  k_buf.at[s * PARTS + c], local_sem.at[c]).wait()

        @pl.when(jnp.logical_not(mine))
        def _():
            k_copy(q, x_send, across).wait_recv()

        @pl.when((side == 0) & (zz <= z) & has_up)
        def _():
            k_copy(q, up_send, up).start()

        @pl.when((side == 0) & (zz >= z) & has_down)
        def _():
            k_copy(q, down_send, down).start()

        @pl.when((side == 0) & jnp.logical_not(skips_x(zz, c)))
        def _():
            k_copy(q, x_send, across).start()

        if line > 1:
            passes = (side == 1) & (zz == z) & (c >= LATE)
            ends = (side == 0) & (c == PARTS - 1)

            @pl.when(passes & up_soon)
            def _():
                k_copy(q, up_send, up).start()

            @pl.when(passes & down_soon)
            def _():
                k_copy(q, down_send, down).start()

            @pl.when(ends & (zz == 0) & up_last)
            def _():
                for k in crossed:
                    k_copy(k, up_send, up).start()

            @pl.when(ends & (zz == line - 1) & down_last)
            def _():
                for k in crossed:
                    k_copy(k, down_send, down).start()

        for b in reversed(range(bits)):
            @pl.when(j_mine)
            def _():
                slice_copy(k_buf.at[q, :, pl.ds(j_off, jw)], j_buf, q, j_send.at[b], j_recv, flip(b)).start()

            if windows == 1:
                @pl.when(b_mine)
                def _():
                    slice_copy(k_buf.at[q, :, pl.ds(b_off, bw)], b_buf, q, b_send.at[b], b_recv, flip(b)).start()
        if windows > 1:
            @pl.when(b_mine)
            def _():
                slice_copy(k_buf.at[q, :, pl.ds(b_off, bw)], b_buf, q, w_send, b_recv, before).start()

    def j_arrive(q):
        slice_copy(k_buf.at[q, :, pl.ds(j_off, jw)], j_buf, q, j_send.at[0], j_recv, flip(0)).wait_recv()

    def b_arrive(q):
        slice_copy(k_buf.at[q, :, pl.ds(b_off, bw)], b_buf, q, b_send.at[0], b_recv, flip(0)).wait_recv()

    j_passes = (j_rel[0] == 0) & jnp.logical_not(j_mine)
    b_passes = b_rel[0] == 0 if windows > 1 else (b_rel[0] == 0) & jnp.logical_not(b_mine)

    def forward(q):
        @pl.when(j_passes)
        def _():
            j_arrive(q)
            for b in reversed(range(bits)):
                @pl.when(sends_on(j_rel, b))
                def _():
                    slice_copy(j_buf.at[q], j_buf, q, j_send.at[b], j_recv, flip(b)).start()

        @pl.when(b_passes)
        def _():
            b_arrive(q)
            for b in reversed(range(bits)):
                @pl.when(sends_on(b_rel, b))
                def _():
                    slice_copy(b_buf.at[q], b_buf, q, b_send.at[b], b_recv, flip(b)).start()

    def ready(q):
        @pl.when(j_rel[0] != 0)
        def _():
            j_arrive(q)

        @pl.when(j_mine)
        def _():
            j_buf[q] = k_buf[q, :, pl.ds(j_off, jw)]

        @pl.when(b_rel[0] != 0)
        def _():
            b_arrive(q)

        if windows == 1:
            @pl.when(b_mine)
            def _():
                b_buf[q] = k_buf[q, :, pl.ds(b_off, bw)]

    def add_stats(stat, block):
        wide = block.astype(jnp.float32).reshape(part_rows // 8, 8, block.shape[-1])
        stat[0] += jnp.sum(wide, axis=0)
        stat[1] += jnp.sum(wide * wide, axis=0)

    def pair(a, b):
        return lax.dot_general(a, b, (((0,), (0,)), ((), ())), preferred_element_type=jnp.float32)

    def compute(q):
        ready(q)
        whole = k_buf[q]
        j_cols = j_buf[q]
        b_cols = b_buf[q]
        add_stats(k_stat, whole)
        add_stats(j_stat, j_cols)
        add_stats(b_stat, b_cols)

        win_out[0] += pair(j_cols, whole)
        band_sum[0] += pair(b_cols, whole)

    def step(o, held):
        side, zz, c, q = item(o)

        @pl.when(o < chunks)
        def _():
            take(side, zz, c, q)

        @pl.when((o >= PASS) & (o < chunks + PASS))
        def _():
            forward(held[PASS - 1])

        @pl.when(o >= USE)
        def _():
            compute(held[USE - 1])

        return (q, *held[:-1])

    lax.fori_loop(0, chunks + USE, step, (jnp.int32(0),) * USE)

    count = jnp.float32(rows * shard_count)

    def moments(total, square):
        mean = total / count
        return mean, 1.0 / jnp.maximum(square / count - mean * mean, VAR_FLOOR)

    row_mean, row_inv = moments(jnp.sum(k_stat[0], axis=0, keepdims=True), jnp.sum(k_stat[1], axis=0, keepdims=True))

    def finish(out, stat, height):
        mean, inv = moments(jnp.sum(stat[0].T, axis=1, keepdims=True), jnp.sum(stat[1].T, axis=1, keepdims=True))
        for a in range(0, height, 64):
            e = min(a + 64, height)
            covar = out[0, a:e] / count - mean[a:e] * row_mean
            out[0, a:e] = covar * covar * (inv[a:e] * row_inv)

    finish(win_out, j_stat, jw)
    finish(band_sum, b_stat, bw)
    if band_wide:
        band_out[0] = band_sum[0, pl.ds(pl.multiple_of((s * band) % bw, band), band)]

    def sent(buf, number, sem):
        part = buf.at[pl.ds(0, number)]
        pltpu.make_async_remote_copy(
            src_ref=part, dst_ref=part, send_sem=sem, recv_sem=k_recv.at[0],
            device_id=across, device_id_type=MESH).wait_send()

    for zz in range(line):
        over = sum(not by_z(zz, a, c) for a in range(line) for c in range(PARTS))

        @pl.when(z == zz)
        def _():
            if zz < line - 1:
                sent(k_buf, (zz + 1) * PARTS + PARTS - LATE, up_send)
            if zz > 0:
                sent(k_buf, (line - zz) * PARTS + PARTS - LATE, down_send)
            sent(k_buf, over, x_send)

    for b in range(bits):
        @pl.when(sends_on(j_rel, b))
        def _():
            sent(j_buf, chunks, j_send.at[b])

        @pl.when(sends_on(b_rel, b))
        def _():
            sent(b_buf, chunks, b_send.at[b])
    if windows > 1:
        @pl.when(b_mine)
        def _():
            sent(b_buf, chunks, w_send)


def shards(dosages):
    rows, width = dosages.shape
    shard_count = lax.axis_size("samp")
    windows = lax.axis_size("win")
    blocks = lax.axis_size("snp")
    jw = width * blocks // shard_count
    band = OV // shard_count
    bw = max(band, 128)
    bits = blocks.bit_length() - 1
    chunks = shard_count * PARTS
    part_rows = rows // PARTS
    sizes = (shard_count, windows, blocks, rows, width, jw, band, bw)
    dma = pltpu.SemaphoreType.DMA
    return pl.pallas_call(
        functools.partial(kernel, sizes),
        out_shape=(
            jax.ShapeDtypeStruct((1, jw, width), jnp.float32),
            jax.ShapeDtypeStruct((1, band, width), jnp.float32),
        ),
        in_specs=[pl.BlockSpec(memory_space=pl.ANY)],
        out_specs=[pl.BlockSpec(memory_space=pltpu.VMEM)] * 2,
        scratch_shapes=[
            pltpu.VMEM((chunks, part_rows, width), jnp.bfloat16),
            pltpu.VMEM((chunks, part_rows, jw), jnp.bfloat16),
            pltpu.VMEM((chunks, part_rows, bw), jnp.bfloat16),
            pltpu.VMEM((2, 8, width), jnp.float32),
            pltpu.VMEM((2, 8, jw), jnp.float32),
            pltpu.VMEM((2, 8, bw), jnp.float32),
            dma((PARTS,)),
            dma((chunks,)), dma, dma, dma,
            dma((chunks,)), dma((bits,)),
            dma((chunks,)), dma((bits,)), dma,
        ] + ([pltpu.VMEM((1, bw, width), jnp.float32)] if bw != band else []),
        compiler_params=pltpu.CompilerParams(
            collective_id=0, has_side_effects=True, vmem_limit_bytes=67043328
        ),
    )(dosages)


def solution(mesh):
    return jax.shard_map(
        shards,
        mesh=mesh,
        in_specs=(P("samp", ("win", "snp")),),
        out_specs=(P("win", "samp", "snp"), P("win", "samp", "snp")),
        check_vma=False,
    )
```

```python
import functools
import heapq

import jax
import jax.numpy as jnp
from jax import lax
from jax.experimental import pallas as pl
from jax.experimental.pallas import tpu as pltpu
from jax.sharding import PartitionSpec as P

OV = 1024
VAR_FLOOR = 0.05
COLS = 2
PARTS = 4
LATE = PARTS // 2
PASS = 2
USE = 4
HEAD_START = 6000
LAST = 2
MESH = pl.DeviceIdType.MESH


def by_z(z, zz, c):
    return c >= LATE and abs(z - zz) == 1


def sends(line, z, item):
    side, zz, c = item
    out = []
    if side == 0:
        if zz <= z and z < line - 1:
            out.append((1, item))
        if zz >= z and z > 0:
            out.append((-1, item))
        if not by_z(z, zz, c):
            out.append((0, item))
        if c == PARTS - 1:
            for way, far in ((-1, line - 1), (1, 0)):
                if zz == far and 0 <= z + way < line and last_on(line, z, way):
                    out += [(way, (1, z, k)) for k in range(LATE, PARTS)]
    elif zz == z and c >= LATE:
        for way in (-1, 1):
            if 0 <= z + way < line and not last_on(line, z, way):
                out.append((way, item))
    return out


def last_on(line, z, way):
    return z < line // 2 if way < 0 else z >= line // 2


def plan(line):
    hop = 1.0
    lag = 0.35
    events = [(0.0, z * PARTS + c, z, (0, z, c)) for z in range(line) for c in range(PARTS)]
    heapq.heapify(events)
    free = {}
    order = [[] for _ in range(line)]
    count = line * PARTS
    while events:
        t, _, z, item = heapq.heappop(events)
        order[z].append(item)
        for way, (side, zz, c) in sends(line, z, item):
            begin = max(free.get((z, way), 0.0), t)
            free[z, way] = begin + hop
            moved = (side, zz, c) if way else (1 - side, zz, c)
            heapq.heappush(events, (begin + hop + lag, count, z + way, moved))
            count += 1
    for z in range(line // 2, line):
        order[z] = [(side, line - 1 - zz, c) for side, zz, c in order[line - 1 - z]]
    return order


def lookup(i, values):
    out = jnp.int32(0)
    for j, v in enumerate(values):
        if v:
            out = out + jnp.where(i == j, jnp.int32(v), jnp.int32(0))
    return out


def kernel(sizes, x_hbm, win_out, band_out, k_buf, j_buf, b_buf, k_stat, j_stat, b_stat,
           local_sem, k_recv, up_send, down_send, x_send, j_recv, j_send, b_recv, b_send, w_send, *band_wide):
    shard_count, windows, blocks, rows, width, jw, band, bw = sizes
    line = shard_count // COLS
    part_rows = rows // PARTS
    bits = blocks.bit_length() - 1
    chunks = shard_count * PARTS
    s = lax.axis_index("samp")
    n = lax.axis_index("snp")
    z = s // COLS
    x = s % COLS
    has_up = z < line - 1
    has_down = z > 0
    up = {"samp": jnp.minimum(s + COLS, shard_count - COLS + x)}
    down = {"samp": jnp.maximum(s - COLS, x)}
    across = {"samp": s + 1 - 2 * x}

    def bit(v, b):
        return (v // (1 << b)) % 2

    def flip(b):
        return {"snp": n + (1 << b) * (1 - 2 * bit(n, b))}

    j_home = (s * jw) // width
    j_off = pl.multiple_of((s * jw) % width, jw)
    b_home = (s * band) // width
    b_off = pl.multiple_of(((s * band) % width) // bw * bw, bw)
    j_rel = [(bit(n, b) + bit(j_home, b)) % 2 for b in range(bits)]
    b_rel = [(bit(n, b) + bit(b_home, b)) % 2 for b in range(bits)]

    def sends_on(rel, b):
        low = jnp.int32(0)
        for a in range(b + 1):
            low = low + rel[a]
        return low == 0

    def is_home(rel):
        total = jnp.int32(0)
        for r in rel:
            total = total + r
        return total == 0

    j_mine = is_home(j_rel)
    b_mine = is_home(b_rel)

    def k_copy(q, sem, to):
        return pltpu.make_async_remote_copy(
            src_ref=k_buf.at[q], dst_ref=k_buf.at[q], send_sem=sem, recv_sem=k_recv.at[q],
            device_id=to, device_id_type=MESH)

    def slice_copy(src, buf, q, send, recv, to):
        return pltpu.make_async_remote_copy(
            src_ref=src, dst_ref=buf.at[q], send_sem=send, recv_sem=recv.at[q],
            device_id=to, device_id_type=MESH)

    order = plan(line)
    band_sum = band_wide[0] if band_wide else band_out
    low = z < line // 2
    near_z = jnp.where(low, z, line - 1 - z)

    def item(o):
        code = jnp.int32(0)
        for half in range((line + 1) // 2):
            mine = lookup(o, [(side * line + zz) * PARTS + c for side, zz, c in order[half]])
            code = code + jnp.where(near_z == half, mine, 0)
        c = code % PARTS
        zz = (code // PARTS) % line
        side = code // (PARTS * line)
        zz = jnp.where(low, zz, line - 1 - zz)
        xx = jnp.where(side == 1, 1 - x, x)
        return side, zz, c, (zz * COLS + xx) * PARTS + c

    def skips_x(zz, c):
        return (c >= LATE) & ((zz == z + 1) | (zz == z - 1))

    crossed = [(s + 1 - 2 * x) * PARTS + c for c in range(LATE, PARTS)]
    up_last = has_up & (z >= line // 2)
    down_last = has_down & (z < line // 2)
    up_soon = has_up & (z < line // 2)
    down_soon = has_down & (z >= line // 2)

    for c in range(PARTS):
        pltpu.make_async_copy(x_hbm.at[pl.ds(c * part_rows, part_rows)],
                              k_buf.at[s * PARTS + c], local_sem.at[c]).start()

    barrier = pltpu.get_barrier_semaphore()

    def greet(to):
        pl.semaphore_signal(barrier, inc=1, device_id=to, device_id_type=MESH)

    pl.when(has_up)(lambda: greet(up))
    pl.when(has_down)(lambda: greet(down))
    greet(across)
    for b in range(bits):
        greet(flip(b))
    expected = 1 + bits
    if windows > 1:
        w = lax.axis_index("win")
        before = {"win": (w + windows - 1) % windows}
        after = {"win": (w + 1) % windows}
        greet(before)
        greet(after)
        expected += 2
    pl.semaphore_wait(barrier, expected + has_up.astype(jnp.int32) + has_down.astype(jnp.int32))

    pl.when((n > 0) & (n < blocks - 1))(lambda: pl.delay(HEAD_START))

    k_stat[...] = jnp.zeros_like(k_stat)
    j_stat[...] = jnp.zeros_like(j_stat)
    b_stat[...] = jnp.zeros_like(b_stat)
    win_out[...] = jnp.zeros_like(win_out)
    band_sum[...] = jnp.zeros_like(band_sum)

    def take(side, zz, c, q):
        mine = (side == 0) & (zz == z)

        @pl.when(mine)
        def _():
            pltpu.make_async_copy(x_hbm.at[pl.ds(c * part_rows, part_rows)],
                                  k_buf.at[s * PARTS + c], local_sem.at[c]).wait()

        @pl.when(jnp.logical_not(mine))
        def _():
            k_copy(q, x_send, across).wait_recv()

        @pl.when((side == 0) & (zz <= z) & has_up)
        def _():
            k_copy(q, up_send, up).start()

        @pl.when((side == 0) & (zz >= z) & has_down)
        def _():
            k_copy(q, down_send, down).start()

        @pl.when((side == 0) & jnp.logical_not(skips_x(zz, c)))
        def _():
            k_copy(q, x_send, across).start()

        if line > 1:
            passes = (side == 1) & (zz == z) & (c >= LATE)
            ends = (side == 0) & (c == PARTS - 1)

            @pl.when(passes & up_soon)
            def _():
                k_copy(q, up_send, up).start()

            @pl.when(passes & down_soon)
            def _():
                k_copy(q, down_send, down).start()

            @pl.when(ends & (zz == 0) & up_last)
            def _():
                for k in crossed:
                    k_copy(k, up_send, up).start()

            @pl.when(ends & (zz == line - 1) & down_last)
            def _():
                for k in crossed:
                    k_copy(k, down_send, down).start()

        for b in reversed(range(bits)):
            @pl.when(j_mine)
            def _():
                slice_copy(k_buf.at[q, :, pl.ds(j_off, jw)], j_buf, q, j_send.at[b], j_recv, flip(b)).start()

            if windows == 1:
                @pl.when(b_mine)
                def _():
                    slice_copy(k_buf.at[q, :, pl.ds(b_off, bw)], b_buf, q, b_send.at[b], b_recv, flip(b)).start()
        if windows > 1:
            @pl.when(b_mine)
            def _():
                slice_copy(k_buf.at[q, :, pl.ds(b_off, bw)], b_buf, q, w_send, b_recv, before).start()

    def j_arrive(q):
        slice_copy(k_buf.at[q, :, pl.ds(j_off, jw)], j_buf, q, j_send.at[0], j_recv, flip(0)).wait_recv()

    def b_arrive(q):
        slice_copy(k_buf.at[q, :, pl.ds(b_off, bw)], b_buf, q, b_send.at[0], b_recv, flip(0)).wait_recv()

    j_passes = (j_rel[0] == 0) & jnp.logical_not(j_mine)
    b_passes = b_rel[0] == 0 if windows > 1 else (b_rel[0] == 0) & jnp.logical_not(b_mine)

    def forward(q):
        @pl.when(j_passes)
        def _():
            j_arrive(q)
            for b in reversed(range(bits)):
                @pl.when(sends_on(j_rel, b))
                def _():
                    slice_copy(j_buf.at[q], j_buf, q, j_send.at[b], j_recv, flip(b)).start()

        @pl.when(b_passes)
        def _():
            b_arrive(q)
            for b in reversed(range(bits)):
                @pl.when(sends_on(b_rel, b))
                def _():
                    slice_copy(b_buf.at[q], b_buf, q, b_send.at[b], b_recv, flip(b)).start()

    def ready(q):
        @pl.when(j_rel[0] != 0)
        def _():
            j_arrive(q)

        @pl.when(j_mine)
        def _():
            j_buf[q] = k_buf[q, :, pl.ds(j_off, jw)]

        @pl.when(b_rel[0] != 0)
        def _():
            b_arrive(q)

        if windows == 1:
            @pl.when(b_mine)
            def _():
                b_buf[q] = k_buf[q, :, pl.ds(b_off, bw)]

    def add_stats(stat, block):
        wide = block.astype(jnp.float32).reshape(part_rows // 8, 8, block.shape[-1])
        stat[0] += jnp.sum(wide, axis=0)
        stat[1] += jnp.sum(wide * wide, axis=0)

    def pair(a, b):
        return lax.dot_general(a, b, (((0,), (0,)), ((), ())), preferred_element_type=jnp.float32)

    def compute(q):
        ready(q)
        whole = k_buf[q]
        j_cols = j_buf[q]
        b_cols = b_buf[q]
        add_stats(k_stat, whole)
        add_stats(j_stat, j_cols)
        add_stats(b_stat, b_cols)

        win_out[0] += pair(j_cols, whole)
        band_sum[0] += pair(b_cols, whole)

    def place(o):
        return item(o)[3]

    def summed(o):
        closing = jnp.maximum(0, o - (chunks - 1 - 2 * (USE - LAST))) // 2
        return jnp.maximum(0, o + 1 - jnp.maximum(LAST, USE - closing))

    def step(o, held):
        side, zz, c, q = item(o)
        take(side, zz, c, q)

        @pl.when(o >= PASS)
        def _():
            forward(held[PASS - 1])

        lax.fori_loop(summed(o - 1), summed(o), lambda i, _: compute(place(i)), None)
        return (q, *held[:-1])

    held = lax.fori_loop(0, chunks, step, (jnp.int32(0),) * PASS)
    for k in reversed(range(PASS)):
        forward(held[k])

    def rest(i, _):
        compute(place(i))

    lax.fori_loop(chunks - LAST, chunks, rest, None)

    count = jnp.float32(rows * shard_count)

    def moments(total, square):
        mean = total / count
        return mean, 1.0 / jnp.maximum(square / count - mean * mean, VAR_FLOOR)

    row_mean, row_inv = moments(jnp.sum(k_stat[0], axis=0, keepdims=True), jnp.sum(k_stat[1], axis=0, keepdims=True))

    def finish(out, stat, height):
        mean, inv = moments(jnp.sum(stat[0].T, axis=1, keepdims=True), jnp.sum(stat[1].T, axis=1, keepdims=True))
        for a in range(0, height, 64):
            e = min(a + 64, height)
            covar = out[0, a:e] / count - mean[a:e] * row_mean
            out[0, a:e] = covar * covar * (inv[a:e] * row_inv)

    finish(win_out, j_stat, jw)
    finish(band_sum, b_stat, bw)
    if band_wide:
        band_out[0] = band_sum[0, pl.ds(pl.multiple_of((s * band) % bw, band), band)]

    def sent(buf, number, sem):
        part = buf.at[pl.ds(0, number)]
        pltpu.make_async_remote_copy(
            src_ref=part, dst_ref=part, send_sem=sem, recv_sem=k_recv.at[0],
            device_id=across, device_id_type=MESH).wait_send()

    for zz in range(line):
        over = sum(not by_z(zz, a, c) for a in range(line) for c in range(PARTS))

        @pl.when(z == zz)
        def _():
            if zz < line - 1:
                sent(k_buf, (zz + 1) * PARTS + PARTS - LATE, up_send)
            if zz > 0:
                sent(k_buf, (line - zz) * PARTS + PARTS - LATE, down_send)
            sent(k_buf, over, x_send)

    for b in range(bits):
        @pl.when(sends_on(j_rel, b))
        def _():
            sent(j_buf, chunks, j_send.at[b])

        @pl.when(sends_on(b_rel, b))
        def _():
            sent(b_buf, chunks, b_send.at[b])
    if windows > 1:
        @pl.when(b_mine)
        def _():
            sent(b_buf, chunks, w_send)


def shards(dosages):
    rows, width = dosages.shape
    shard_count = lax.axis_size("samp")
    windows = lax.axis_size("win")
    blocks = lax.axis_size("snp")
    jw = width * blocks // shard_count
    band = OV // shard_count
    bw = max(band, 128)
    bits = blocks.bit_length() - 1
    chunks = shard_count * PARTS
    part_rows = rows // PARTS
    sizes = (shard_count, windows, blocks, rows, width, jw, band, bw)
    dma = pltpu.SemaphoreType.DMA
    return pl.pallas_call(
        functools.partial(kernel, sizes),
        out_shape=(
            jax.ShapeDtypeStruct((1, jw, width), jnp.float32),
            jax.ShapeDtypeStruct((1, band, width), jnp.float32),
        ),
        in_specs=[pl.BlockSpec(memory_space=pl.ANY)],
        out_specs=[pl.BlockSpec(memory_space=pltpu.VMEM)] * 2,
        scratch_shapes=[
            pltpu.VMEM((chunks, part_rows, width), jnp.bfloat16),
            pltpu.VMEM((chunks, part_rows, jw), jnp.bfloat16),
            pltpu.VMEM((chunks, part_rows, bw), jnp.bfloat16),
            pltpu.VMEM((2, 8, width), jnp.float32),
            pltpu.VMEM((2, 8, jw), jnp.float32),
            pltpu.VMEM((2, 8, bw), jnp.float32),
            dma((PARTS,)),
            dma((chunks,)), dma, dma, dma,
            dma((chunks,)), dma((bits,)),
            dma((chunks,)), dma((bits,)), dma,
        ] + ([pltpu.VMEM((1, bw, width), jnp.float32)] if bw != band else []),
        compiler_params=pltpu.CompilerParams(
            collective_id=0, has_side_effects=True, vmem_limit_bytes=24 * 2**20
        ),
    )(dosages)


def solution(mesh):
    return jax.shard_map(
        shards,
        mesh=mesh,
        in_specs=(P("samp", ("win", "snp")),),
        out_specs=(P("win", "samp", "snp"), P("win", "samp", "snp")),
        check_vma=False,
    )
```

```python
import functools
import heapq

import jax
import jax.numpy as jnp
from jax import lax
from jax.experimental import pallas as pl
from jax.experimental.pallas import tpu as pltpu
from jax.sharding import PartitionSpec as P

OV = 1024
VAR_FLOOR = 0.05
COLS = 2
PARTS = 4
LATE = PARTS // 2
PASS = 2
USE = 4
HEAD_START = 5000
TILE = 64
CLOSE = 4
END = 3
MESH = pl.DeviceIdType.MESH


def by_z(z, zz, c):
    return c >= LATE and abs(z - zz) == 1


def sends(line, z, item):
    side, zz, c = item
    out = []
    if side == 0:
        if zz <= z and z < line - 1:
            out.append((1, item))
        if zz >= z and z > 0:
            out.append((-1, item))
        if not by_z(z, zz, c):
            out.append((0, item))
        if c == PARTS - 1:
            for way, far in ((-1, line - 1), (1, 0)):
                if zz == far and 0 <= z + way < line and last_on(line, z, way):
                    out += [(way, (1, z, k)) for k in range(LATE, PARTS)]
    elif zz == z and c >= LATE:
        for way in (-1, 1):
            if 0 <= z + way < line and not last_on(line, z, way):
                out.append((way, item))
    return out


def last_on(line, z, way):
    return z < line // 2 if way < 0 else z >= line // 2


def plan(line):
    hop = 1.0
    lag = 0.35
    events = [(0.0, z * PARTS + c, z, (0, z, c)) for z in range(line) for c in range(PARTS)]
    heapq.heapify(events)
    free = {}
    order = [[] for _ in range(line)]
    count = line * PARTS
    while events:
        t, _, z, item = heapq.heappop(events)
        order[z].append(item)
        for way, (side, zz, c) in sends(line, z, item):
            begin = max(free.get((z, way), 0.0), t)
            free[z, way] = begin + hop
            moved = (side, zz, c) if way else (1 - side, zz, c)
            heapq.heappush(events, (begin + hop + lag, count, z + way, moved))
            count += 1
    for z in range(line // 2, line):
        order[z] = [(side, line - 1 - zz, c) for side, zz, c in order[line - 1 - z]]
    return order


def lookup(i, values):
    out = jnp.int32(0)
    for j, v in enumerate(values):
        if v:
            out = out + jnp.where(i == j, jnp.int32(v), jnp.int32(0))
    return out


def kernel(sizes, x_hbm, win_sum, band_sum, k_stat, j_stat, b_stat, k_buf, j_buf, b_buf,
           local_sem, k_recv, up_send, down_send, x_send, j_recv, j_send, b_recv, b_send, w_send):
    shard_count, windows, blocks, rows, width, jw, band, bw = sizes
    line = shard_count // COLS
    part_rows = rows // PARTS
    bits = blocks.bit_length() - 1
    chunks = shard_count * PARTS
    s = lax.axis_index("samp")
    n = lax.axis_index("snp")
    z = s // COLS
    x = s % COLS
    has_up = z < line - 1
    has_down = z > 0
    up = {"samp": jnp.minimum(s + COLS, shard_count - COLS + x)}
    down = {"samp": jnp.maximum(s - COLS, x)}
    across = {"samp": s + 1 - 2 * x}

    def bit(v, b):
        return (v // (1 << b)) % 2

    def flip(b):
        return {"snp": n + (1 << b) * (1 - 2 * bit(n, b))}

    j_home = (s * jw) // width
    j_off = pl.multiple_of((s * jw) % width, jw)
    b_home = (s * band) // width
    b_off = pl.multiple_of(((s * band) % width) // bw * bw, bw)
    j_rel = [(bit(n, b) + bit(j_home, b)) % 2 for b in range(bits)]
    b_rel = [(bit(n, b) + bit(b_home, b)) % 2 for b in range(bits)]

    def sends_on(rel, b):
        low = jnp.int32(0)
        for a in range(b + 1):
            low = low + rel[a]
        return low == 0

    def is_home(rel):
        total = jnp.int32(0)
        for r in rel:
            total = total + r
        return total == 0

    j_mine = is_home(j_rel)
    b_mine = is_home(b_rel)

    def k_copy(q, sem, to):
        return pltpu.make_async_remote_copy(
            src_ref=k_buf.at[q], dst_ref=k_buf.at[q], send_sem=sem, recv_sem=k_recv.at[q],
            device_id=to, device_id_type=MESH)

    def slice_copy(src, buf, q, send, recv, to):
        return pltpu.make_async_remote_copy(
            src_ref=src, dst_ref=buf.at[q], send_sem=send, recv_sem=recv.at[q],
            device_id=to, device_id_type=MESH)

    order = plan(line)
    low = z < line // 2
    near_z = jnp.where(low, z, line - 1 - z)

    def item(o):
        code = jnp.int32(0)
        for half in range((line + 1) // 2):
            mine = lookup(o, [(side * line + zz) * PARTS + c for side, zz, c in order[half]])
            code = code + jnp.where(near_z == half, mine, 0)
        c = code % PARTS
        zz = (code // PARTS) % line
        side = code // (PARTS * line)
        zz = jnp.where(low, zz, line - 1 - zz)
        xx = jnp.where(side == 1, 1 - x, x)
        return side, zz, c, (zz * COLS + xx) * PARTS + c

    def skips_x(zz, c):
        return (c >= LATE) & ((zz == z + 1) | (zz == z - 1))

    crossed = [(s + 1 - 2 * x) * PARTS + c for c in range(LATE, PARTS)]
    up_last = has_up & (z >= line // 2)
    down_last = has_down & (z < line // 2)
    up_soon = has_up & (z < line // 2)
    down_soon = has_down & (z >= line // 2)

    for c in range(PARTS):
        pltpu.make_async_copy(x_hbm.at[pl.ds(c * part_rows, part_rows)],
                              k_buf.at[s * PARTS + c], local_sem.at[c]).start()

    barrier = pltpu.get_barrier_semaphore()

    def greet(to):
        pl.semaphore_signal(barrier, inc=1, device_id=to, device_id_type=MESH)

    pl.when(has_up)(lambda: greet(up))
    pl.when(has_down)(lambda: greet(down))
    greet(across)
    for b in range(bits):
        greet(flip(b))
    expected = 1 + bits
    if windows > 1:
        w = lax.axis_index("win")
        before = {"win": (w + windows - 1) % windows}
        after = {"win": (w + 1) % windows}
        greet(before)
        greet(after)
        expected += 2
    pl.semaphore_wait(barrier, expected + has_up.astype(jnp.int32) + has_down.astype(jnp.int32))

    pl.when((n > 0) & (n < blocks - 1))(lambda: pl.delay(HEAD_START))

    k_stat[...] = jnp.zeros_like(k_stat)
    j_stat[...] = jnp.zeros_like(j_stat)
    b_stat[...] = jnp.zeros_like(b_stat)
    win_sum[...] = jnp.zeros_like(win_sum)
    band_sum[...] = jnp.zeros_like(band_sum)

    def take(side, zz, c, q):
        mine = (side == 0) & (zz == z)

        @pl.when(mine)
        def _():
            pltpu.make_async_copy(x_hbm.at[pl.ds(c * part_rows, part_rows)],
                                  k_buf.at[s * PARTS + c], local_sem.at[c]).wait()

        @pl.when(jnp.logical_not(mine))
        def _():
            k_copy(q, x_send, across).wait_recv()

        @pl.when((side == 0) & (zz <= z) & has_up)
        def _():
            k_copy(q, up_send, up).start()

        @pl.when((side == 0) & (zz >= z) & has_down)
        def _():
            k_copy(q, down_send, down).start()

        @pl.when((side == 0) & jnp.logical_not(skips_x(zz, c)))
        def _():
            k_copy(q, x_send, across).start()

        if line > 1:
            passes = (side == 1) & (zz == z) & (c >= LATE)
            ends = (side == 0) & (c == PARTS - 1)

            @pl.when(passes & up_soon)
            def _():
                k_copy(q, up_send, up).start()

            @pl.when(passes & down_soon)
            def _():
                k_copy(q, down_send, down).start()

            @pl.when(ends & (zz == 0) & up_last)
            def _():
                for k in crossed:
                    k_copy(k, up_send, up).start()

            @pl.when(ends & (zz == line - 1) & down_last)
            def _():
                for k in crossed:
                    k_copy(k, down_send, down).start()

        for b in reversed(range(bits)):
            @pl.when(j_mine)
            def _():
                slice_copy(k_buf.at[q, :, pl.ds(j_off, jw)], j_buf, q, j_send.at[b], j_recv, flip(b)).start()

            if windows == 1:
                @pl.when(b_mine)
                def _():
                    slice_copy(k_buf.at[q, :, pl.ds(b_off, bw)], b_buf, q, b_send.at[b], b_recv, flip(b)).start()
        if windows > 1:
            @pl.when(b_mine)
            def _():
                slice_copy(k_buf.at[q, :, pl.ds(b_off, bw)], b_buf, q, w_send, b_recv, before).start()

    def j_arrive(q):
        slice_copy(k_buf.at[q, :, pl.ds(j_off, jw)], j_buf, q, j_send.at[0], j_recv, flip(0)).wait_recv()

    def b_arrive(q):
        slice_copy(k_buf.at[q, :, pl.ds(b_off, bw)], b_buf, q, b_send.at[0], b_recv, flip(0)).wait_recv()

    j_passes = (j_rel[0] == 0) & jnp.logical_not(j_mine)
    b_passes = b_rel[0] == 0 if windows > 1 else (b_rel[0] == 0) & jnp.logical_not(b_mine)

    def forward(q):
        @pl.when(j_passes)
        def _():
            j_arrive(q)
            for b in reversed(range(bits)):
                @pl.when(sends_on(j_rel, b))
                def _():
                    slice_copy(j_buf.at[q], j_buf, q, j_send.at[b], j_recv, flip(b)).start()

        @pl.when(b_passes)
        def _():
            b_arrive(q)
            for b in reversed(range(bits)):
                @pl.when(sends_on(b_rel, b))
                def _():
                    slice_copy(b_buf.at[q], b_buf, q, b_send.at[b], b_recv, flip(b)).start()

    def add_stats(stat, block):
        wide = block.astype(jnp.float32).reshape(part_rows // 8, 8, block.shape[-1])
        stat[0] += jnp.sum(wide, axis=0)
        stat[1] += jnp.sum(wide * wide, axis=0)

    def pair(a, b):
        return lax.dot_general(a, b, (((0,), (0,)), ((), ())), preferred_element_type=jnp.float32)

    def compute(q):
        @pl.when(j_rel[0] != 0)
        def _():
            j_arrive(q)

        @pl.when(j_mine)
        def _():
            j_buf[q] = k_buf[q, :, pl.ds(j_off, jw)]

        @pl.when(b_rel[0] != 0)
        def _():
            b_arrive(q)

        if windows == 1:
            @pl.when(b_mine)
            def _():
                b_buf[q] = k_buf[q, :, pl.ds(b_off, bw)]

        whole = k_buf[q]
        j_cols = j_buf[q]
        b_cols = b_buf[q]
        add_stats(k_stat, whole)
        add_stats(j_stat, j_cols)
        add_stats(b_stat, b_cols)
        win_sum[0] += pair(j_cols, whole)
        band_sum[0] += pair(b_cols, whole)

    def place(o):
        return item(o)[3]

    def each(first, last, what):
        def one(i, _):
            what(place(i))

        lax.fori_loop(first, last, one, None)

    def summed(o):
        return jnp.maximum(0, o + 1 - USE)

    def step(o, held):
        side, zz, c, q = item(o)
        take(side, zz, c, q)

        @pl.when(o >= PASS)
        def _():
            forward(held[PASS - 1])

        each(summed(o - 1), summed(o), compute)
        return (q, *held[:-1])

    at_end = (z == 0) | (z == line - 1)
    eager = at_end & (j_home == b_home)
    closing = chunks - CLOSE
    lax.fori_loop(0, closing, step, (jnp.int32(0),) * PASS)

    def passed(o):
        return jnp.where(o < closing, closing - PASS, jnp.where(eager, o, o - 1))

    def summed_in(o):
        lag = jnp.where(eager, 0, jnp.where(at_end, END, USE))
        return jnp.where(o < closing, closing - USE, o - lag)

    def close(o, _):
        each(passed(o - 1), passed(o), forward)
        each(summed_in(o - 1), summed_in(o), compute)
        take(*item(o))

    lax.fori_loop(closing, chunks, close, None)
    each(passed(chunks - 1), chunks, forward)
    each(summed_in(chunks - 1), chunks, compute)

    def sent(buf, number, sem):
        part = buf.at[pl.ds(0, number)]
        pltpu.make_async_remote_copy(
            src_ref=part, dst_ref=part, send_sem=sem, recv_sem=k_recv.at[0],
            device_id=across, device_id_type=MESH).wait_send()

    for zz in range(line):
        over = sum(not by_z(zz, a, c) for a in range(line) for c in range(PARTS))

        @pl.when(z == zz)
        def _():
            if zz < line - 1:
                sent(k_buf, (zz + 1) * PARTS + PARTS - LATE, up_send)
            if zz > 0:
                sent(k_buf, (line - zz) * PARTS + PARTS - LATE, down_send)
            sent(k_buf, over, x_send)

    for b in range(bits):
        @pl.when(sends_on(j_rel, b))
        def _():
            sent(j_buf, chunks, j_send.at[b])

        @pl.when(sends_on(b_rel, b))
        def _():
            sent(b_buf, chunks, b_send.at[b])
    if windows > 1:
        @pl.when(b_mine)
        def _():
            sent(b_buf, chunks, w_send)


def finish(sizes, win_sum, band_sum, k_stat, j_stat, b_stat, win_out, band_out, win_buf, band_buf, sems):
    shard_count, windows, blocks, rows, width, jw, band, bw = sizes
    count = jnp.float32(rows * shard_count)
    off = (lax.axis_index("samp") * band) % bw

    def moments(total, square):
        mean = total / count
        return mean, 1.0 / jnp.maximum(square / count - mean * mean, VAR_FLOOR)

    row_mean, row_inv = moments(jnp.sum(k_stat[0], axis=0, keepdims=True), jnp.sum(k_stat[1], axis=0, keepdims=True))

    def squares(total, stat, buf, height, copy):
        mean, inv = moments(jnp.sum(stat[0].T, axis=1, keepdims=True), jnp.sum(stat[1].T, axis=1, keepdims=True))
        for a in range(0, height, TILE):
            e = a + TILE
            covar = total[0, a:e] / count - mean[a:e] * row_mean
            buf[a:e] = covar * covar * (inv[a:e] * row_inv)
            copy(a // TILE)

    def win_copy(t):
        return pltpu.make_async_copy(
            win_buf.at[pl.ds(t * TILE, TILE)], win_out.at[0, pl.ds(t * TILE, TILE)], sems.at[t])

    band_copy = pltpu.make_async_copy(
        band_buf.at[pl.ds(pl.multiple_of(off, 8), band)], band_out.at[0], sems.at[jw // TILE])
    squares(win_sum, j_stat, win_buf, jw, lambda t: win_copy(t).start())
    squares(band_sum, b_stat, band_buf, bw, lambda t: None)
    band_copy.start()
    for t in range(jw // TILE):
        win_copy(t).wait()
    band_copy.wait()


def shards(dosages):
    rows, width = dosages.shape
    shard_count = lax.axis_size("samp")
    windows = lax.axis_size("win")
    blocks = lax.axis_size("snp")
    jw = width * blocks // shard_count
    band = OV // shard_count
    bw = max(band, 128)
    bits = blocks.bit_length() - 1
    chunks = shard_count * PARTS
    part_rows = rows // PARTS
    sizes = (shard_count, windows, blocks, rows, width, jw, band, bw)
    dma = pltpu.SemaphoreType.DMA
    f32 = jnp.float32
    sums = (
        jax.ShapeDtypeStruct((1, jw, width), f32),
        jax.ShapeDtypeStruct((1, bw, width), f32),
        jax.ShapeDtypeStruct((2, 8, width), f32),
        jax.ShapeDtypeStruct((2, 8, jw), f32),
        jax.ShapeDtypeStruct((2, 8, bw), f32),
    )
    parts = pl.pallas_call(
        functools.partial(kernel, sizes),
        out_shape=sums,
        in_specs=[pl.BlockSpec(memory_space=pl.ANY)],
        out_specs=[pl.BlockSpec(memory_space=pltpu.VMEM)] * len(sums),
        scratch_shapes=[
            pltpu.VMEM((chunks, part_rows, width), jnp.bfloat16),
            pltpu.VMEM((chunks, part_rows, jw), jnp.bfloat16),
            pltpu.VMEM((chunks, part_rows, bw), jnp.bfloat16),
            dma((PARTS,)),
            dma((chunks,)), dma, dma, dma,
            dma((chunks,)), dma((bits,)),
            dma((chunks,)), dma((bits,)), dma,
        ],
        compiler_params=pltpu.CompilerParams(
            collective_id=0, has_side_effects=True, vmem_limit_bytes=24 * 2**20
        ),
    )(dosages)
    return pl.pallas_call(
        functools.partial(finish, sizes),
        out_shape=(
            jax.ShapeDtypeStruct((1, jw, width), f32),
            jax.ShapeDtypeStruct((1, band, width), f32),
        ),
        in_specs=[pl.BlockSpec(memory_space=pltpu.VMEM)] * len(sums),
        out_specs=[pl.BlockSpec(memory_space=pl.ANY)] * 2,
        scratch_shapes=[
            pltpu.VMEM((jw, width), f32),
            pltpu.VMEM((bw, width), f32),
            dma((jw // TILE + 1,)),
        ],
        compiler_params=pltpu.CompilerParams(vmem_limit_bytes=24 * 2**20),
    )(*parts)


def solution(mesh):
    return jax.shard_map(
        shards,
        mesh=mesh,
        in_specs=(P("samp", ("win", "snp")),),
        out_specs=(P("win", "samp", "snp"), P("win", "samp", "snp")),
        check_vma=False,
    )
```

```python
import functools
import heapq

import jax
import jax.numpy as jnp
from jax import lax
from jax.experimental import pallas as pl
from jax.experimental.pallas import tpu as pltpu
from jax.sharding import PartitionSpec as P

OV = 1024
VAR_FLOOR = 0.05
COLS = 2
PARTS = 4
LATE = PARTS // 2
PASS = 2
USE = 4
HEAD_START = 6000
TILE = 64
CLOSE = 4
END = 3
MESH = pl.DeviceIdType.MESH


def by_z(z, zz, c):
    return c >= LATE and abs(z - zz) == 1


def sends(line, z, item):
    side, zz, c = item
    out = []
    if side == 0:
        if zz <= z and z < line - 1:
            out.append((1, item))
        if zz >= z and z > 0:
            out.append((-1, item))
        if not by_z(z, zz, c):
            out.append((0, item))
        if c == PARTS - 1:
            for way, far in ((-1, line - 1), (1, 0)):
                if zz == far and 0 <= z + way < line and last_on(line, z, way):
                    out += [(way, (1, z, k)) for k in range(LATE, PARTS)]
    elif zz == z and c >= LATE:
        for way in (-1, 1):
            if 0 <= z + way < line and not last_on(line, z, way):
                out.append((way, item))
    return out


def last_on(line, z, way):
    return z < line // 2 if way < 0 else z >= line // 2


def plan(line):
    hop = 1.0
    lag = 0.35
    events = [(0.0, z * PARTS + c, z, (0, z, c)) for z in range(line) for c in range(PARTS)]
    heapq.heapify(events)
    free = {}
    order = [[] for _ in range(line)]
    count = line * PARTS
    while events:
        t, _, z, item = heapq.heappop(events)
        order[z].append(item)
        for way, (side, zz, c) in sends(line, z, item):
            begin = max(free.get((z, way), 0.0), t)
            free[z, way] = begin + hop
            moved = (side, zz, c) if way else (1 - side, zz, c)
            heapq.heappush(events, (begin + hop + lag, count, z + way, moved))
            count += 1
    for z in range(line // 2, line):
        order[z] = [(side, line - 1 - zz, c) for side, zz, c in order[line - 1 - z]]
    return order


def lookup(i, values):
    out = jnp.int32(0)
    for j, v in enumerate(values):
        if v:
            out = out + jnp.where(i == j, jnp.int32(v), jnp.int32(0))
    return out


def kernel(sizes, x_hbm, win_sum, band_sum, k_stat, j_stat, b_stat, k_buf, j_buf, b_buf,
           local_sem, k_recv, up_send, down_send, x_send, j_recv, j_send, b_recv, b_send, w_send):
    shard_count, windows, blocks, rows, width, jw, band, bw = sizes
    line = shard_count // COLS
    part_rows = rows // PARTS
    bits = blocks.bit_length() - 1
    chunks = shard_count * PARTS
    s = lax.axis_index("samp")
    n = lax.axis_index("snp")
    z = s // COLS
    x = s % COLS
    has_up = z < line - 1
    has_down = z > 0
    up = {"samp": jnp.minimum(s + COLS, shard_count - COLS + x)}
    down = {"samp": jnp.maximum(s - COLS, x)}
    across = {"samp": s + 1 - 2 * x}

    def bit(v, b):
        return (v // (1 << b)) % 2

    def flip(b):
        return {"snp": n + (1 << b) * (1 - 2 * bit(n, b))}

    def beside(delta):
        to = n
        for b in range(bits):
            if delta >> b & 1:
                to = to + (1 << b) * (1 - 2 * bit(n, b))
        return {"snp": to}

    j_home = (s * jw) // width
    j_off = pl.multiple_of((s * jw) % width, jw)
    b_home = (s * band) // width
    b_off = pl.multiple_of(((s * band) % width) // bw * bw, bw)
    j_rel = [(bit(n, b) + bit(j_home, b)) % 2 for b in range(bits)]

    def sends_on(rel, b):
        low = jnp.int32(0)
        for a in range(b + 1):
            low = low + rel[a]
        return low == 0

    def is_home(rel):
        total = jnp.int32(0)
        for r in rel:
            total = total + r
        return total == 0

    j_mine = is_home(j_rel)
    b_mine = n == b_home

    def k_copy(q, sem, to):
        return pltpu.make_async_remote_copy(
            src_ref=k_buf.at[q], dst_ref=k_buf.at[q], send_sem=sem, recv_sem=k_recv.at[q],
            device_id=to, device_id_type=MESH)

    def slice_copy(src, buf, q, send, recv, to):
        return pltpu.make_async_remote_copy(
            src_ref=src, dst_ref=buf.at[q], send_sem=send, recv_sem=recv.at[q],
            device_id=to, device_id_type=MESH)

    order = plan(line)
    low = z < line // 2
    near_z = jnp.where(low, z, line - 1 - z)

    def item(o):
        code = jnp.int32(0)
        for half in range((line + 1) // 2):
            mine = lookup(o, [(side * line + zz) * PARTS + c for side, zz, c in order[half]])
            code = code + jnp.where(near_z == half, mine, 0)
        c = code % PARTS
        zz = (code // PARTS) % line
        side = code // (PARTS * line)
        zz = jnp.where(low, zz, line - 1 - zz)
        xx = jnp.where(side == 1, 1 - x, x)
        return side, zz, c, (zz * COLS + xx) * PARTS + c

    def skips_x(zz, c):
        return (c >= LATE) & ((zz == z + 1) | (zz == z - 1))

    crossed = [(s + 1 - 2 * x) * PARTS + c for c in range(LATE, PARTS)]
    up_last = has_up & (z >= line // 2)
    down_last = has_down & (z < line // 2)
    up_soon = has_up & (z < line // 2)
    down_soon = has_down & (z >= line // 2)

    for c in range(PARTS):
        pltpu.make_async_copy(x_hbm.at[pl.ds(c * part_rows, part_rows)],
                              k_buf.at[s * PARTS + c], local_sem.at[c]).start()

    barrier = pltpu.get_barrier_semaphore()

    def greet(to):
        pl.semaphore_signal(barrier, inc=1, device_id=to, device_id_type=MESH)

    pl.when(has_up)(lambda: greet(up))
    pl.when(has_down)(lambda: greet(down))
    greet(across)
    for delta in range(1, blocks):
        greet(beside(delta))
    expected = blocks
    if windows > 1:
        w = lax.axis_index("win")
        before = {"win": (w + windows - 1) % windows}
        after = {"win": (w + 1) % windows}
        greet(before)
        greet(after)
        expected += 2
    pl.semaphore_wait(barrier, expected + has_up.astype(jnp.int32) + has_down.astype(jnp.int32))

    pl.when((n > 0) & (n < blocks - 1))(lambda: pl.delay(HEAD_START))

    k_stat[...] = jnp.zeros_like(k_stat)
    j_stat[...] = jnp.zeros_like(j_stat)
    b_stat[...] = jnp.zeros_like(b_stat)
    win_sum[...] = jnp.zeros_like(win_sum)
    band_sum[...] = jnp.zeros_like(band_sum)

    def take(side, zz, c, q):
        mine = (side == 0) & (zz == z)

        @pl.when(mine)
        def _():
            pltpu.make_async_copy(x_hbm.at[pl.ds(c * part_rows, part_rows)],
                                  k_buf.at[s * PARTS + c], local_sem.at[c]).wait()

        @pl.when(jnp.logical_not(mine))
        def _():
            k_copy(q, x_send, across).wait_recv()

        @pl.when((side == 0) & (zz <= z) & has_up)
        def _():
            k_copy(q, up_send, up).start()

        @pl.when((side == 0) & (zz >= z) & has_down)
        def _():
            k_copy(q, down_send, down).start()

        @pl.when((side == 0) & jnp.logical_not(skips_x(zz, c)))
        def _():
            k_copy(q, x_send, across).start()

        if line > 1:
            passes = (side == 1) & (zz == z) & (c >= LATE)
            ends = (side == 0) & (c == PARTS - 1)

            @pl.when(passes & up_soon)
            def _():
                k_copy(q, up_send, up).start()

            @pl.when(passes & down_soon)
            def _():
                k_copy(q, down_send, down).start()

            @pl.when(ends & (zz == 0) & up_last)
            def _():
                for k in crossed:
                    k_copy(k, up_send, up).start()

            @pl.when(ends & (zz == line - 1) & down_last)
            def _():
                for k in crossed:
                    k_copy(k, down_send, down).start()

        for b in reversed(range(bits)):
            @pl.when(j_mine)
            def _():
                slice_copy(k_buf.at[q, :, pl.ds(j_off, jw)], j_buf, q, j_send.at[b], j_recv, flip(b)).start()

        if windows == 1:
            @pl.when(b_mine)
            def _():
                for delta in reversed(range(1, blocks)):
                    slice_copy(k_buf.at[q, :, pl.ds(b_off, bw)], b_buf, q, b_send.at[delta - 1], b_recv,
                               beside(delta)).start()
        if windows > 1:
            @pl.when(b_mine)
            def _():
                slice_copy(k_buf.at[q, :, pl.ds(b_off, bw)], b_buf, q, w_send, b_recv, before).start()

    def j_arrive(q):
        slice_copy(k_buf.at[q, :, pl.ds(j_off, jw)], j_buf, q, j_send.at[0], j_recv, flip(0)).wait_recv()

    def b_arrive(q):
        slice_copy(k_buf.at[q, :, pl.ds(b_off, bw)], b_buf, q, b_send.at[0], b_recv, flip(0)).wait_recv()

    j_passes = (j_rel[0] == 0) & jnp.logical_not(j_mine)

    def forward(q):
        @pl.when(j_passes)
        def _():
            j_arrive(q)
            for b in reversed(range(bits)):
                @pl.when(sends_on(j_rel, b))
                def _():
                    slice_copy(j_buf.at[q], j_buf, q, j_send.at[b], j_recv, flip(b)).start()

        if windows > 1:
            @pl.when(b_mine)
            def _():
                b_arrive(q)
                for delta in reversed(range(1, blocks)):
                    slice_copy(b_buf.at[q], b_buf, q, b_send.at[delta - 1], b_recv, beside(delta)).start()

    def add_stats(stat, block):
        wide = block.astype(jnp.float32).reshape(part_rows // 8, 8, block.shape[-1])
        stat[0] += jnp.sum(wide, axis=0)
        stat[1] += jnp.sum(wide * wide, axis=0)

    def pair(a, b):
        return lax.dot_general(a, b, (((0,), (0,)), ((), ())), preferred_element_type=jnp.float32)

    def compute(q):
        @pl.when(j_rel[0] != 0)
        def _():
            j_arrive(q)

        @pl.when(j_mine)
        def _():
            j_buf[q] = k_buf[q, :, pl.ds(j_off, jw)]

        @pl.when(jnp.logical_not(b_mine))
        def _():
            b_arrive(q)

        if windows == 1:
            @pl.when(b_mine)
            def _():
                b_buf[q] = k_buf[q, :, pl.ds(b_off, bw)]

        whole = k_buf[q]
        j_cols = j_buf[q]
        b_cols = b_buf[q]
        add_stats(k_stat, whole)
        add_stats(j_stat, j_cols)
        add_stats(b_stat, b_cols)
        win_sum[0] += pair(j_cols, whole)
        band_sum[0] += pair(b_cols, whole)

    def place(o):
        return item(o)[3]

    def each(first, last, what):
        def one(i, _):
            what(place(i))

        lax.fori_loop(first, last, one, None)

    def summed(o):
        return jnp.maximum(0, o + 1 - USE)

    def step(o, held):
        side, zz, c, q = item(o)
        take(side, zz, c, q)

        @pl.when(o >= PASS)
        def _():
            forward(held[PASS - 1])

        each(summed(o - 1), summed(o), compute)
        return (q, *held[:-1])

    at_end = (z == 0) | (z == line - 1)
    eager = at_end & (j_home == b_home)
    closing = chunks - CLOSE
    lax.fori_loop(0, closing, step, (jnp.int32(0),) * PASS)

    def passed(o):
        return jnp.where(o < closing, closing - PASS, jnp.where(eager, o, o - 1))

    def summed_in(o):
        lag = jnp.where(eager, 0, jnp.where(at_end, END, USE))
        return jnp.where(o < closing, closing - USE, o - lag)

    def close(o, _):
        each(passed(o - 1), passed(o), forward)
        each(summed_in(o - 1), summed_in(o), compute)
        take(*item(o))

    lax.fori_loop(closing, chunks, close, None)
    begun = summed_in(chunks - 1)
    each(passed(chunks - 1), chunks - 1, forward)
    each(begun, chunks - 1, compute)
    each(chunks - 1, chunks, forward)
    each(chunks - 1, chunks, compute)

    def sent(buf, number, sem):
        part = buf.at[pl.ds(0, number)]
        pltpu.make_async_remote_copy(
            src_ref=part, dst_ref=part, send_sem=sem, recv_sem=k_recv.at[0],
            device_id=across, device_id_type=MESH).wait_send()

    for zz in range(line):
        over = sum(not by_z(zz, a, c) for a in range(line) for c in range(PARTS))

        @pl.when(z == zz)
        def _():
            if zz < line - 1:
                sent(k_buf, (zz + 1) * PARTS + PARTS - LATE, up_send)
            if zz > 0:
                sent(k_buf, (line - zz) * PARTS + PARTS - LATE, down_send)
            sent(k_buf, over, x_send)

    for b in range(bits):
        @pl.when(sends_on(j_rel, b))
        def _():
            sent(j_buf, chunks, j_send.at[b])

    @pl.when(b_mine)
    def _():
        for delta in range(1, blocks):
            sent(b_buf, chunks, b_send.at[delta - 1])
        if windows > 1:
            sent(b_buf, chunks, w_send)


def finish(sizes, win_sum, band_sum, k_stat, j_stat, b_stat, win_out, band_out, win_buf, band_buf, sems):
    shard_count, windows, blocks, rows, width, jw, band, bw = sizes
    count = jnp.float32(rows * shard_count)
    off = (lax.axis_index("samp") * band) % bw

    def moments(total, square):
        mean = total / count
        return mean, 1.0 / jnp.maximum(square / count - mean * mean, VAR_FLOOR)

    row_mean, row_inv = moments(jnp.sum(k_stat[0], axis=0, keepdims=True), jnp.sum(k_stat[1], axis=0, keepdims=True))

    def squares(total, stat, buf, height, copy):
        both = moments(jnp.sum(stat[0], axis=0, keepdims=True), jnp.sum(stat[1], axis=0, keepdims=True))
        both = jnp.concatenate([both[0]] * 4 + [both[1]] * 4, axis=0).T
        mean, inv = both[:, 0:1], both[:, 4:5]
        for a in range(0, height, TILE):
            e = a + TILE
            covar = total[0, a:e] / count - mean[a:e] * row_mean
            buf[a:e] = covar * covar * (inv[a:e] * row_inv)
            copy(a // TILE)

    def win_copy(t):
        return pltpu.make_async_copy(
            win_buf.at[pl.ds(t * TILE, TILE)], win_out.at[0, pl.ds(t * TILE, TILE)], sems.at[t])

    band_copy = pltpu.make_async_copy(
        band_buf.at[pl.ds(pl.multiple_of(off, 8), band)], band_out.at[0], sems.at[jw // TILE])
    squares(win_sum, j_stat, win_buf, jw, lambda t: win_copy(t).start())
    squares(band_sum, b_stat, band_buf, bw, lambda t: None)
    band_copy.start()
    for t in range(jw // TILE):
        win_copy(t).wait()
    band_copy.wait()


def shards(dosages):
    rows, width = dosages.shape
    shard_count = lax.axis_size("samp")
    windows = lax.axis_size("win")
    blocks = lax.axis_size("snp")
    jw = width * blocks // shard_count
    band = OV // shard_count
    bw = max(band, 128)
    bits = blocks.bit_length() - 1
    chunks = shard_count * PARTS
    part_rows = rows // PARTS
    sizes = (shard_count, windows, blocks, rows, width, jw, band, bw)
    dma = pltpu.SemaphoreType.DMA
    f32 = jnp.float32
    sums = (
        jax.ShapeDtypeStruct((1, jw, width), f32),
        jax.ShapeDtypeStruct((1, bw, width), f32),
        jax.ShapeDtypeStruct((2, 8, width), f32),
        jax.ShapeDtypeStruct((2, 8, jw), f32),
        jax.ShapeDtypeStruct((2, 8, bw), f32),
    )
    parts = pl.pallas_call(
        functools.partial(kernel, sizes),
        out_shape=sums,
        in_specs=[pl.BlockSpec(memory_space=pl.ANY)],
        out_specs=[pl.BlockSpec(memory_space=pltpu.VMEM)] * len(sums),
        scratch_shapes=[
            pltpu.VMEM((chunks, part_rows, width), jnp.bfloat16),
            pltpu.VMEM((chunks, part_rows, jw), jnp.bfloat16),
            pltpu.VMEM((chunks, part_rows, bw), jnp.bfloat16),
            dma((PARTS,)),
            dma((chunks,)), dma, dma, dma,
            dma((chunks,)), dma((bits,)),
            dma((chunks,)), dma((blocks - 1,)), dma,
        ],
        compiler_params=pltpu.CompilerParams(
            collective_id=0, has_side_effects=True, vmem_limit_bytes=24 * 2**20
        ),
    )(dosages)
    return pl.pallas_call(
        functools.partial(finish, sizes),
        out_shape=(
            jax.ShapeDtypeStruct((1, jw, width), f32),
            jax.ShapeDtypeStruct((1, band, width), f32),
        ),
        in_specs=[pl.BlockSpec(memory_space=pltpu.VMEM)] * len(sums),
        out_specs=[pl.BlockSpec(memory_space=pl.ANY)] * 2,
        scratch_shapes=[
            pltpu.VMEM((jw, width), f32),
            pltpu.VMEM((bw, width), f32),
            dma((jw // TILE + 1,)),
        ],
        compiler_params=pltpu.CompilerParams(vmem_limit_bytes=24 * 2**20),
    )(*parts)


def solution(mesh):
    return jax.shard_map(
        shards,
        mesh=mesh,
        in_specs=(P("samp", ("win", "snp")),),
        out_specs=(P("win", "samp", "snp"), P("win", "samp", "snp")),
        check_vma=False,
    )
```

```python
import functools
import heapq

import jax
import jax.numpy as jnp
from jax import lax
from jax.experimental import pallas as pl
from jax.experimental.pallas import tpu as pltpu
from jax.sharding import PartitionSpec as P

OV = 1024
VAR_FLOOR = 0.05
COLS = 2
PARTS = 4
LATE = PARTS // 2
PASS = 2
USE = 4
HEAD_START = 6000
TILE = 64
CLOSE = 4
END = 3
MESH = pl.DeviceIdType.MESH


def by_z(z, zz, c):
    return c >= LATE and abs(z - zz) == 1


def sends(line, z, item):
    side, zz, c = item
    out = []
    if side == 0:
        if zz <= z and z < line - 1:
            out.append((1, item))
        if zz >= z and z > 0:
            out.append((-1, item))
        if not by_z(z, zz, c):
            out.append((0, item))
        if c == PARTS - 1:
            for way, far in ((-1, line - 1), (1, 0)):
                if zz == far and 0 <= z + way < line and last_on(line, z, way):
                    out += [(way, (1, z, k)) for k in range(LATE, PARTS)]
    elif zz == z and c >= LATE:
        for way in (-1, 1):
            if 0 <= z + way < line and not last_on(line, z, way):
                out.append((way, item))
    return out


def last_on(line, z, way):
    return z < line // 2 if way < 0 else z >= line // 2


def plan(line):
    hop = 1.0
    lag = 0.35
    events = [(0.0, z * PARTS + c, z, (0, z, c)) for z in range(line) for c in range(PARTS)]
    heapq.heapify(events)
    free = {}
    order = [[] for _ in range(line)]
    count = line * PARTS
    while events:
        t, _, z, item = heapq.heappop(events)
        order[z].append(item)
        for way, (side, zz, c) in sends(line, z, item):
            begin = max(free.get((z, way), 0.0), t)
            free[z, way] = begin + hop
            moved = (side, zz, c) if way else (1 - side, zz, c)
            heapq.heappush(events, (begin + hop + lag, count, z + way, moved))
            count += 1
    for z in range(line // 2, line):
        order[z] = [(side, line - 1 - zz, c) for side, zz, c in order[line - 1 - z]]
    return order


def lookup(i, values):
    out = jnp.int32(0)
    for j, v in enumerate(values):
        if v:
            out = out + jnp.where(i == j, jnp.int32(v), jnp.int32(0))
    return out


def kernel(sizes, x_hbm, win_sum, band_sum, k_stat, j_stat, b_stat, k_buf, j_buf, b_buf,
           local_sem, k_recv, up_send, down_send, x_send, j_recv, j_send, b_recv, b_send, w_send):
    shard_count, windows, blocks, rows, width, jw, band, bw = sizes
    line = shard_count // COLS
    part_rows = rows // PARTS
    bits = blocks.bit_length() - 1
    chunks = shard_count * PARTS
    s = lax.axis_index("samp")
    n = lax.axis_index("snp")
    z = s // COLS
    x = s % COLS
    has_up = z < line - 1
    has_down = z > 0
    up = {"samp": jnp.minimum(s + COLS, shard_count - COLS + x)}
    down = {"samp": jnp.maximum(s - COLS, x)}
    across = {"samp": s + 1 - 2 * x}

    def bit(v, b):
        return (v // (1 << b)) % 2

    def flip(b):
        return {"snp": n + (1 << b) * (1 - 2 * bit(n, b))}

    def beside(delta):
        to = n
        for b in range(bits):
            if delta >> b & 1:
                to = to + (1 << b) * (1 - 2 * bit(n, b))
        return {"snp": to}

    j_home = (s * jw) // width
    j_off = pl.multiple_of((s * jw) % width, jw)
    b_home = (s * band) // width
    b_off = pl.multiple_of(((s * band) % width) // bw * bw, bw)
    j_rel = [(bit(n, b) + bit(j_home, b)) % 2 for b in range(bits)]

    def sends_on(rel, b):
        low = jnp.int32(0)
        for a in range(b + 1):
            low = low + rel[a]
        return low == 0

    def is_home(rel):
        total = jnp.int32(0)
        for r in rel:
            total = total + r
        return total == 0

    j_mine = is_home(j_rel)
    b_mine = n == b_home

    def k_copy(q, sem, to, src=None):
        return pltpu.make_async_remote_copy(
            src_ref=k_buf.at[q] if src is None else src, dst_ref=k_buf.at[q], send_sem=sem, recv_sem=k_recv.at[q],
            device_id=to, device_id_type=MESH)

    def slice_copy(src, buf, q, send, recv, to):
        return pltpu.make_async_remote_copy(
            src_ref=src, dst_ref=buf.at[q], send_sem=send, recv_sem=recv.at[q],
            device_id=to, device_id_type=MESH)

    order = plan(line)
    low = z < line // 2
    near_z = jnp.where(low, z, line - 1 - z)

    def item(o):
        code = jnp.int32(0)
        for half in range((line + 1) // 2):
            mine = lookup(o, [(side * line + zz) * PARTS + c for side, zz, c in order[half]])
            code = code + jnp.where(near_z == half, mine, 0)
        c = code % PARTS
        zz = (code // PARTS) % line
        side = code // (PARTS * line)
        zz = jnp.where(low, zz, line - 1 - zz)
        xx = jnp.where(side == 1, 1 - x, x)
        return side, zz, c, (zz * COLS + xx) * PARTS + c

    def skips_x(zz, c):
        return (c >= LATE) & ((zz == z + 1) | (zz == z - 1))

    crossed = [(s + 1 - 2 * x) * PARTS + c for c in range(LATE, PARTS)]
    up_last = has_up & (z >= line // 2)
    down_last = has_down & (z < line // 2)
    up_soon = has_up & (z < line // 2)
    down_soon = has_down & (z >= line // 2)

    for c in range(PARTS):
        pltpu.make_async_copy(x_hbm.at[pl.ds(c * part_rows, part_rows)],
                              k_buf.at[s * PARTS + c], local_sem.at[c]).start()

    barrier = pltpu.get_barrier_semaphore()

    def greet(to):
        pl.semaphore_signal(barrier, inc=1, device_id=to, device_id_type=MESH)

    pl.when(has_up)(lambda: greet(up))
    pl.when(has_down)(lambda: greet(down))
    greet(across)
    for delta in range(1, blocks):
        greet(beside(delta))
    expected = blocks
    if windows > 1:
        w = lax.axis_index("win")
        before = {"win": (w + windows - 1) % windows}
        after = {"win": (w + 1) % windows}
        greet(before)
        greet(after)
        expected += 2
    pl.semaphore_wait(barrier, expected + has_up.astype(jnp.int32) + has_down.astype(jnp.int32))

    pl.when((n > 0) & (n < blocks - 1))(lambda: pl.delay(HEAD_START))

    k_stat[...] = jnp.zeros_like(k_stat)
    j_stat[...] = jnp.zeros_like(j_stat)
    b_stat[...] = jnp.zeros_like(b_stat)
    win_sum[...] = jnp.zeros_like(win_sum)
    band_sum[...] = jnp.zeros_like(band_sum)

    def take(side, zz, c, q):
        mine = (side == 0) & (zz == z)

        @pl.when(mine)
        def _():
            own = x_hbm.at[pl.ds(c * part_rows, part_rows)]
            pl.when(has_up)(lambda: k_copy(q, up_send, up, own).start())
            pl.when(has_down)(lambda: k_copy(q, down_send, down, own).start())
            k_copy(q, x_send, across, own).start()
            pltpu.make_async_copy(own, k_buf.at[q], local_sem.at[c]).wait()

        @pl.when(jnp.logical_not(mine))
        def _():
            k_copy(q, x_send, across).wait_recv()

        @pl.when((side == 0) & (zz < z) & has_up)
        def _():
            k_copy(q, up_send, up).start()

        @pl.when((side == 0) & (zz > z) & has_down)
        def _():
            k_copy(q, down_send, down).start()

        @pl.when((side == 0) & (zz != z) & jnp.logical_not(skips_x(zz, c)))
        def _():
            k_copy(q, x_send, across).start()

        if line > 1:
            passes = (side == 1) & (zz == z) & (c >= LATE)
            ends = (side == 0) & (c == PARTS - 1)

            @pl.when(passes & up_soon)
            def _():
                k_copy(q, up_send, up).start()

            @pl.when(passes & down_soon)
            def _():
                k_copy(q, down_send, down).start()

            @pl.when(ends & (zz == 0) & up_last)
            def _():
                for k in crossed:
                    k_copy(k, up_send, up).start()

            @pl.when(ends & (zz == line - 1) & down_last)
            def _():
                for k in crossed:
                    k_copy(k, down_send, down).start()

        for b in reversed(range(bits)):
            @pl.when(j_mine)
            def _():
                slice_copy(k_buf.at[q, :, pl.ds(j_off, jw)], j_buf, q, j_send.at[b], j_recv, flip(b)).start()

        if windows == 1:
            @pl.when(b_mine)
            def _():
                for delta in reversed(range(1, blocks)):
                    slice_copy(k_buf.at[q, :, pl.ds(b_off, bw)], b_buf, q, b_send.at[delta - 1], b_recv,
                               beside(delta)).start()
        if windows > 1:
            @pl.when(b_mine)
            def _():
                slice_copy(k_buf.at[q, :, pl.ds(b_off, bw)], b_buf, q, w_send, b_recv, before).start()

    def j_arrive(q):
        slice_copy(k_buf.at[q, :, pl.ds(j_off, jw)], j_buf, q, j_send.at[0], j_recv, flip(0)).wait_recv()

    def b_arrive(q):
        slice_copy(k_buf.at[q, :, pl.ds(b_off, bw)], b_buf, q, b_send.at[0], b_recv, flip(0)).wait_recv()

    j_passes = (j_rel[0] == 0) & jnp.logical_not(j_mine)

    def forward(q):
        @pl.when(j_passes)
        def _():
            j_arrive(q)
            for b in reversed(range(bits)):
                @pl.when(sends_on(j_rel, b))
                def _():
                    slice_copy(j_buf.at[q], j_buf, q, j_send.at[b], j_recv, flip(b)).start()

        if windows > 1:
            @pl.when(b_mine)
            def _():
                b_arrive(q)
                for delta in reversed(range(1, blocks)):
                    slice_copy(b_buf.at[q], b_buf, q, b_send.at[delta - 1], b_recv, beside(delta)).start()

    def add_stats(stat, block):
        wide = block.astype(jnp.float32).reshape(block.shape[0] // 8, 8, block.shape[-1])
        stat[0] += jnp.sum(wide, axis=0)
        stat[1] += jnp.sum(wide * wide, axis=0)

    def pair(a, b):
        return lax.dot_general(a, b, (((0,), (0,)), ((), ())), preferred_element_type=jnp.float32)

    def arrive(q):
        @pl.when(j_rel[0] != 0)
        def _():
            j_arrive(q)

        @pl.when(j_mine)
        def _():
            j_buf[q] = k_buf[q, :, pl.ds(j_off, jw)]

        @pl.when(jnp.logical_not(b_mine))
        def _():
            b_arrive(q)

        if windows == 1:
            @pl.when(b_mine)
            def _():
                b_buf[q] = k_buf[q, :, pl.ds(b_off, bw)]

    def compute(*places):
        for q in places:
            arrive(q)
        whole, j_cols, b_cols = (
            jnp.concatenate([buf[q] for q in places], axis=0) for buf in (k_buf, j_buf, b_buf))
        add_stats(k_stat, whole)
        add_stats(j_stat, j_cols)
        add_stats(b_stat, b_cols)
        win_sum[0] += pair(j_cols, whole)
        band_sum[0] += pair(b_cols, whole)

    def place(o):
        return item(o)[3]

    def each(first, last, what):
        def one(i, _):
            what(place(i))

        lax.fori_loop(first, last, one, None)

    def summed(o):
        return jnp.maximum(0, o + 1 - USE)

    def step(o, held):
        side, zz, c, q = item(o)
        take(side, zz, c, q)

        @pl.when(o >= PASS)
        def _():
            forward(held[PASS - 1])

        each(summed(o - 1), summed(o), compute)
        return (q, *held[:-1])

    at_end = (z == 0) | (z == line - 1)
    eager = at_end & (j_home == b_home)
    closing = chunks - CLOSE
    lax.fori_loop(0, closing, step, (jnp.int32(0),) * PASS)

    def passed(o):
        return jnp.where(o < closing, closing - PASS, jnp.where(eager, o, o - 1))

    def summed_in(o):
        lag = jnp.where(eager, 0, jnp.where(at_end, END, USE))
        last = jnp.where(eager, chunks - 2, chunks - 4)
        return jnp.where(o < closing, closing - USE, jnp.where(o == chunks - 1, last, o - lag))

    def close(o, _):
        each(passed(o - 1), passed(o), forward)
        each(summed_in(o - 1), summed_in(o), compute)
        take(*item(o))

    lax.fori_loop(closing, chunks, close, None)
    def two(i, _):
        compute(place(2 * i), place(2 * i + 1))

    each(passed(chunks - 1), chunks - 1, forward)
    lax.fori_loop(summed_in(chunks - 1) // 2, chunks // 2 - 1, two, None)
    each(chunks - 1, chunks, forward)
    lax.fori_loop(chunks // 2 - 1, chunks // 2, two, None)

    def sent(buf, number, sem):
        part = buf.at[pl.ds(0, number)]
        pltpu.make_async_remote_copy(
            src_ref=part, dst_ref=part, send_sem=sem, recv_sem=k_recv.at[0],
            device_id=across, device_id_type=MESH).wait_send()

    for zz in range(line):
        over = sum(not by_z(zz, a, c) for a in range(line) for c in range(PARTS))

        @pl.when(z == zz)
        def _():
            if zz < line - 1:
                sent(k_buf, (zz + 1) * PARTS + PARTS - LATE, up_send)
            if zz > 0:
                sent(k_buf, (line - zz) * PARTS + PARTS - LATE, down_send)
            sent(k_buf, over, x_send)

    for b in range(bits):
        @pl.when(sends_on(j_rel, b))
        def _():
            sent(j_buf, chunks, j_send.at[b])

    @pl.when(b_mine)
    def _():
        for delta in range(1, blocks):
            sent(b_buf, chunks, b_send.at[delta - 1])
        if windows > 1:
            sent(b_buf, chunks, w_send)


def finish(sizes, win_sum, band_sum, k_stat, j_stat, b_stat, win_out, band_out, win_buf, band_buf, sems):
    shard_count, windows, blocks, rows, width, jw, band, bw = sizes
    count = jnp.float32(rows * shard_count)
    off = (lax.axis_index("samp") * band) % bw

    def moments(total, square):
        mean = total / count
        return mean, 1.0 / jnp.maximum(square / count - mean * mean, VAR_FLOOR)

    row_mean, row_inv = moments(jnp.sum(k_stat[0], axis=0, keepdims=True), jnp.sum(k_stat[1], axis=0, keepdims=True))

    def squares(total, stat, buf, height, copy):
        both = moments(jnp.sum(stat[0], axis=0, keepdims=True), jnp.sum(stat[1], axis=0, keepdims=True))
        both = jnp.concatenate([both[0]] * 4 + [both[1]] * 4, axis=0).T
        mean, inv = both[:, 0:1], both[:, 4:5]
        for a in range(0, height, TILE):
            e = a + TILE
            covar = total[0, a:e] / count - mean[a:e] * row_mean
            buf[a:e] = covar * covar * (inv[a:e] * row_inv)
            copy(a // TILE)

    def win_copy(t):
        return pltpu.make_async_copy(
            win_buf.at[pl.ds(t * TILE, TILE)], win_out.at[0, pl.ds(t * TILE, TILE)], sems.at[t])

    band_copy = pltpu.make_async_copy(
        band_buf.at[pl.ds(pl.multiple_of(off, 8), band)], band_out.at[0], sems.at[jw // TILE])
    squares(win_sum, j_stat, win_buf, jw, lambda t: win_copy(t).start())
    squares(band_sum, b_stat, band_buf, bw, lambda t: None)
    band_copy.start()
    for t in range(jw // TILE):
        win_copy(t).wait()
    band_copy.wait()


def shards(dosages):
    rows, width = dosages.shape
    shard_count = lax.axis_size("samp")
    windows = lax.axis_size("win")
    blocks = lax.axis_size("snp")
    jw = width * blocks // shard_count
    band = OV // shard_count
    bw = max(band, 128)
    bits = blocks.bit_length() - 1
    chunks = shard_count * PARTS
    part_rows = rows // PARTS
    sizes = (shard_count, windows, blocks, rows, width, jw, band, bw)
    dma = pltpu.SemaphoreType.DMA
    f32 = jnp.float32
    sums = (
        jax.ShapeDtypeStruct((1, jw, width), f32),
        jax.ShapeDtypeStruct((1, bw, width), f32),
        jax.ShapeDtypeStruct((2, 8, width), f32),
        jax.ShapeDtypeStruct((2, 8, jw), f32),
        jax.ShapeDtypeStruct((2, 8, bw), f32),
    )
    parts = pl.pallas_call(
        functools.partial(kernel, sizes),
        out_shape=sums,
        in_specs=[pl.BlockSpec(memory_space=pl.ANY)],
        out_specs=[pl.BlockSpec(memory_space=pltpu.VMEM)] * len(sums),
        scratch_shapes=[
            pltpu.VMEM((chunks, part_rows, width), jnp.bfloat16),
            pltpu.VMEM((chunks, part_rows, jw), jnp.bfloat16),
            pltpu.VMEM((chunks, part_rows, bw), jnp.bfloat16),
            dma((PARTS,)),
            dma((chunks,)), dma, dma, dma,
            dma((chunks,)), dma((bits,)),
            dma((chunks,)), dma((blocks - 1,)), dma,
        ],
        compiler_params=pltpu.CompilerParams(
            collective_id=0, has_side_effects=True, vmem_limit_bytes=24 * 2**20
        ),
    )(dosages)
    return pl.pallas_call(
        functools.partial(finish, sizes),
        out_shape=(
            jax.ShapeDtypeStruct((1, jw, width), f32),
            jax.ShapeDtypeStruct((1, band, width), f32),
        ),
        in_specs=[pl.BlockSpec(memory_space=pltpu.VMEM)] * len(sums),
        out_specs=[pl.BlockSpec(memory_space=pl.ANY)] * 2,
        scratch_shapes=[
            pltpu.VMEM((jw, width), f32),
            pltpu.VMEM((bw, width), f32),
            dma((jw // TILE + 1,)),
        ],
        compiler_params=pltpu.CompilerParams(vmem_limit_bytes=24 * 2**20),
    )(*parts)


def solution(mesh):
    return jax.shard_map(
        shards,
        mesh=mesh,
        in_specs=(P("samp", ("win", "snp")),),
        out_specs=(P("win", "samp", "snp"), P("win", "samp", "snp")),
        check_vma=False,
    )
```

```python
import functools
import heapq

import jax
import jax.numpy as jnp
from jax import lax
from jax.experimental import pallas as pl
from jax.experimental.pallas import tpu as pltpu
from jax.sharding import PartitionSpec as P

OV = 1024
VAR_FLOOR = 0.05
COLS = 2
PARTS = 4
LATE = PARTS // 2
PASS = 2
USE = 4
HEAD_START = 6000
TILE = 64
CLOSE = 4
END = 2
MESH = pl.DeviceIdType.MESH


def by_z(z, zz, c):
    return c >= LATE and abs(z - zz) == 1


def sends(line, z, item):
    side, zz, c = item
    out = []
    if side == 0:
        if zz <= z and z < line - 1:
            out.append((1, item))
        if zz >= z and z > 0:
            out.append((-1, item))
        if not by_z(z, zz, c):
            out.append((0, item))
        if c == PARTS - 1:
            for way, far in ((-1, line - 1), (1, 0)):
                if zz == far and 0 <= z + way < line and last_on(line, z, way):
                    out += [(way, (1, z, k)) for k in range(LATE, PARTS)]
    elif zz == z and c >= LATE:
        for way in (-1, 1):
            if 0 <= z + way < line and not last_on(line, z, way):
                out.append((way, item))
    return out


def last_on(line, z, way):
    return z < line // 2 if way < 0 else z >= line // 2


def plan(line):
    hop = 1.0
    lag = 0.35
    events = [(0.0, z * PARTS + c, z, (0, z, c)) for z in range(line) for c in range(PARTS)]
    heapq.heapify(events)
    free = {}
    order = [[] for _ in range(line)]
    count = line * PARTS
    while events:
        t, _, z, item = heapq.heappop(events)
        order[z].append(item)
        for way, (side, zz, c) in sends(line, z, item):
            begin = max(free.get((z, way), 0.0), t)
            free[z, way] = begin + hop
            moved = (side, zz, c) if way else (1 - side, zz, c)
            heapq.heappush(events, (begin + hop + lag, count, z + way, moved))
            count += 1
    for z in range(line // 2, line):
        order[z] = [(side, line - 1 - zz, c) for side, zz, c in order[line - 1 - z]]
    return order


def lookup(i, values):
    out = jnp.int32(0)
    for j, v in enumerate(values):
        if v:
            out = out + jnp.where(i == j, jnp.int32(v), jnp.int32(0))
    return out


def kernel(sizes, x_hbm, win_sum, band_sum, k_stat, j_stat, b_stat, k_buf, j_buf, b_buf,
           local_sem, k_recv, up_send, down_send, x_send, j_recv, j_send, b_recv, b_send, w_send):
    shard_count, windows, blocks, rows, width, jw, band, bw = sizes
    line = shard_count // COLS
    part_rows = rows // PARTS
    bits = blocks.bit_length() - 1
    chunks = shard_count * PARTS
    s = lax.axis_index("samp")
    n = lax.axis_index("snp")
    z = s // COLS
    x = s % COLS
    has_up = z < line - 1
    has_down = z > 0
    up = {"samp": jnp.minimum(s + COLS, shard_count - COLS + x)}
    down = {"samp": jnp.maximum(s - COLS, x)}
    across = {"samp": s + 1 - 2 * x}

    def bit(v, b):
        return (v // (1 << b)) % 2

    def flip(b):
        return {"snp": n + (1 << b) * (1 - 2 * bit(n, b))}

    def beside(delta):
        to = n
        for b in range(bits):
            if delta >> b & 1:
                to = to + (1 << b) * (1 - 2 * bit(n, b))
        return {"snp": to}

    j_home = (s * jw) // width
    j_off = pl.multiple_of((s * jw) % width, jw)
    b_home = (s * band) // width
    b_off = pl.multiple_of(((s * band) % width) // bw * bw, bw)
    j_rel = [(bit(n, b) + bit(j_home, b)) % 2 for b in range(bits)]

    def sends_on(rel, b):
        low = jnp.int32(0)
        for a in range(b + 1):
            low = low + rel[a]
        return low == 0

    def is_home(rel):
        total = jnp.int32(0)
        for r in rel:
            total = total + r
        return total == 0

    j_mine = is_home(j_rel)
    b_mine = n == b_home

    def k_copy(q, sem, to, src=None):
        return pltpu.make_async_remote_copy(
            src_ref=k_buf.at[q] if src is None else src, dst_ref=k_buf.at[q], send_sem=sem, recv_sem=k_recv.at[q],
            device_id=to, device_id_type=MESH)

    def slice_copy(src, buf, q, send, recv, to):
        return pltpu.make_async_remote_copy(
            src_ref=src, dst_ref=buf.at[q], send_sem=send, recv_sem=recv.at[q],
            device_id=to, device_id_type=MESH)

    order = plan(line)
    low = z < line // 2
    near_z = jnp.where(low, z, line - 1 - z)

    def item(o):
        code = jnp.int32(0)
        for half in range((line + 1) // 2):
            mine = lookup(o, [(side * line + zz) * PARTS + c for side, zz, c in order[half]])
            code = code + jnp.where(near_z == half, mine, 0)
        c = code % PARTS
        zz = (code // PARTS) % line
        side = code // (PARTS * line)
        zz = jnp.where(low, zz, line - 1 - zz)
        xx = jnp.where(side == 1, 1 - x, x)
        return side, zz, c, (zz * COLS + xx) * PARTS + c

    def skips_x(zz, c):
        return (c >= LATE) & ((zz == z + 1) | (zz == z - 1))

    crossed = [(s + 1 - 2 * x) * PARTS + c for c in range(LATE, PARTS)]
    up_last = has_up & (z >= line // 2)
    down_last = has_down & (z < line // 2)
    up_soon = has_up & (z < line // 2)
    down_soon = has_down & (z >= line // 2)

    for c in range(PARTS):
        pltpu.make_async_copy(x_hbm.at[pl.ds(c * part_rows, part_rows)],
                              k_buf.at[s * PARTS + c], local_sem.at[c]).start()

    barrier = pltpu.get_barrier_semaphore()

    def greet(to):
        pl.semaphore_signal(barrier, inc=1, device_id=to, device_id_type=MESH)

    pl.when(has_up)(lambda: greet(up))
    pl.when(has_down)(lambda: greet(down))
    greet(across)
    for delta in range(1, blocks):
        greet(beside(delta))
    expected = blocks
    if windows > 1:
        w = lax.axis_index("win")
        before = {"win": (w + windows - 1) % windows}
        after = {"win": (w + 1) % windows}
        greet(before)
        greet(after)
        expected += 2
    pl.semaphore_wait(barrier, expected + has_up.astype(jnp.int32) + has_down.astype(jnp.int32))

    pl.when((n > 0) & (n < blocks - 1))(lambda: pl.delay(HEAD_START))

    k_stat[...] = jnp.zeros_like(k_stat)
    j_stat[...] = jnp.zeros_like(j_stat)
    b_stat[...] = jnp.zeros_like(b_stat)
    win_sum[...] = jnp.zeros_like(win_sum)
    band_sum[...] = jnp.zeros_like(band_sum)

    def take(side, zz, c, q):
        mine = (side == 0) & (zz == z)

        @pl.when(mine)
        def _():
            own = x_hbm.at[pl.ds(c * part_rows, part_rows)]
            pl.when(has_up)(lambda: k_copy(q, up_send, up, own).start())
            pl.when(has_down)(lambda: k_copy(q, down_send, down, own).start())
            k_copy(q, x_send, across, own).start()
            pltpu.make_async_copy(own, k_buf.at[q], local_sem.at[c]).wait()

        @pl.when(jnp.logical_not(mine))
        def _():
            k_copy(q, x_send, across).wait_recv()

        @pl.when((side == 0) & (zz < z) & has_up)
        def _():
            k_copy(q, up_send, up).start()

        @pl.when((side == 0) & (zz > z) & has_down)
        def _():
            k_copy(q, down_send, down).start()

        @pl.when((side == 0) & (zz != z) & jnp.logical_not(skips_x(zz, c)))
        def _():
            k_copy(q, x_send, across).start()

        if line > 1:
            passes = (side == 1) & (zz == z) & (c >= LATE)
            ends = (side == 0) & (c == PARTS - 1)

            @pl.when(passes & up_soon)
            def _():
                k_copy(q, up_send, up).start()

            @pl.when(passes & down_soon)
            def _():
                k_copy(q, down_send, down).start()

            @pl.when(ends & (zz == 0) & up_last)
            def _():
                for k in crossed:
                    k_copy(k, up_send, up).start()

            @pl.when(ends & (zz == line - 1) & down_last)
            def _():
                for k in crossed:
                    k_copy(k, down_send, down).start()

        for b in reversed(range(bits)):
            @pl.when(j_mine)
            def _():
                slice_copy(k_buf.at[q, :, pl.ds(j_off, jw)], j_buf, q, j_send.at[b], j_recv, flip(b)).start()

        if windows == 1:
            @pl.when(b_mine)
            def _():
                for delta in reversed(range(1, blocks)):
                    slice_copy(k_buf.at[q, :, pl.ds(b_off, bw)], b_buf, q, b_send.at[delta - 1], b_recv,
                               beside(delta)).start()
        if windows > 1:
            @pl.when(b_mine)
            def _():
                slice_copy(k_buf.at[q, :, pl.ds(b_off, bw)], b_buf, q, w_send, b_recv, before).start()

    def j_arrive(q):
        slice_copy(k_buf.at[q, :, pl.ds(j_off, jw)], j_buf, q, j_send.at[0], j_recv, flip(0)).wait_recv()

    def b_arrive(q):
        slice_copy(k_buf.at[q, :, pl.ds(b_off, bw)], b_buf, q, b_send.at[0], b_recv, flip(0)).wait_recv()

    j_passes = (j_rel[0] == 0) & jnp.logical_not(j_mine)

    def forward(q):
        @pl.when(j_passes)
        def _():
            j_arrive(q)
            for b in reversed(range(bits)):
                @pl.when(sends_on(j_rel, b))
                def _():
                    slice_copy(j_buf.at[q], j_buf, q, j_send.at[b], j_recv, flip(b)).start()

        if windows > 1:
            @pl.when(b_mine)
            def _():
                b_arrive(q)
                for delta in reversed(range(1, blocks)):
                    slice_copy(b_buf.at[q], b_buf, q, b_send.at[delta - 1], b_recv, beside(delta)).start()

    def add_stats(stat, block):
        wide = block.astype(jnp.float32).reshape(block.shape[0] // 8, 8, block.shape[-1])
        stat[0] += jnp.sum(wide, axis=0)
        stat[1] += jnp.sum(wide * wide, axis=0)

    def pair(a, b):
        return lax.dot_general(a, b, (((0,), (0,)), ((), ())), preferred_element_type=jnp.float32)

    def arrive(q):
        @pl.when(j_rel[0] != 0)
        def _():
            j_arrive(q)

        @pl.when(j_mine)
        def _():
            j_buf[q] = k_buf[q, :, pl.ds(j_off, jw)]

        @pl.when(jnp.logical_not(b_mine))
        def _():
            b_arrive(q)

        if windows == 1:
            @pl.when(b_mine)
            def _():
                b_buf[q] = k_buf[q, :, pl.ds(b_off, bw)]

    def compute(*places):
        for q in places:
            arrive(q)
        whole, j_cols, b_cols = (
            jnp.concatenate([buf[q] for q in places], axis=0) for buf in (k_buf, j_buf, b_buf))
        add_stats(k_stat, whole)
        add_stats(j_stat, j_cols)
        add_stats(b_stat, b_cols)
        win_sum[0] += pair(j_cols, whole)
        band_sum[0] += pair(b_cols, whole)

    def place(o):
        return item(o)[3]

    def each(first, last, what):
        def one(i, _):
            what(place(i))

        lax.fori_loop(first, last, one, None)

    def two(i, _):
        compute(place(2 * i), place(2 * i + 1))

    def add_up(first, last):
        lax.fori_loop(first // 2, last // 2, two, None)

    def summed(o):
        return jnp.maximum(0, o + 1 - USE)

    def step(o, held):
        side, zz, c, q = item(o)
        take(side, zz, c, q)

        @pl.when(o >= PASS)
        def _():
            forward(held[PASS - 1])

        add_up(summed(o - 1), summed(o))
        return (q, *held[:-1])

    at_end = (z == 0) | (z == line - 1)
    eager = at_end & (j_home == b_home)
    closing = chunks - CLOSE
    lax.fori_loop(0, closing, step, (jnp.int32(0),) * PASS)

    def passed(o):
        return jnp.where(o < closing, closing - PASS, jnp.where(eager, o, o - 1))

    def summed_in(o):
        lag = jnp.where(eager, 0, jnp.where(at_end, END, USE))
        last = jnp.where(eager, chunks - 2, chunks - 4)
        return jnp.where(o < closing, closing - USE, jnp.where(o == chunks - 1, last, o - lag))

    def close(o, _):
        each(passed(o - 1), passed(o), forward)
        add_up(summed_in(o - 1), summed_in(o))
        take(*item(o))

    lax.fori_loop(closing, chunks, close, None)
    each(passed(chunks - 1), chunks - 1, forward)
    add_up(summed_in(chunks - 1), chunks - 2)
    each(chunks - 1, chunks, forward)
    add_up(chunks - 2, chunks)

    def sent(buf, number, sem):
        part = buf.at[pl.ds(0, number)]
        pltpu.make_async_remote_copy(
            src_ref=part, dst_ref=part, send_sem=sem, recv_sem=k_recv.at[0],
            device_id=across, device_id_type=MESH).wait_send()

    for zz in range(line):
        over = sum(not by_z(zz, a, c) for a in range(line) for c in range(PARTS))

        @pl.when(z == zz)
        def _():
            if zz < line - 1:
                sent(k_buf, (zz + 1) * PARTS + PARTS - LATE, up_send)
            if zz > 0:
                sent(k_buf, (line - zz) * PARTS + PARTS - LATE, down_send)
            sent(k_buf, over, x_send)

    for b in range(bits):
        @pl.when(sends_on(j_rel, b))
        def _():
            sent(j_buf, chunks, j_send.at[b])

    @pl.when(b_mine)
    def _():
        for delta in range(1, blocks):
            sent(b_buf, chunks, b_send.at[delta - 1])
        if windows > 1:
            sent(b_buf, chunks, w_send)


def finish(sizes, win_sum, band_sum, k_stat, j_stat, b_stat, win_out, band_out, win_buf, band_buf, sems):
    shard_count, windows, blocks, rows, width, jw, band, bw = sizes
    count = jnp.float32(rows * shard_count)
    off = (lax.axis_index("samp") * band) % bw

    def moments(total, square):
        mean = total / count
        return mean, 1.0 / jnp.maximum(square / count - mean * mean, VAR_FLOOR)

    row_mean, row_inv = moments(jnp.sum(k_stat[0], axis=0, keepdims=True), jnp.sum(k_stat[1], axis=0, keepdims=True))

    def squares(total, stat, buf, height, copy):
        both = moments(jnp.sum(stat[0], axis=0, keepdims=True), jnp.sum(stat[1], axis=0, keepdims=True))
        both = jnp.concatenate([both[0]] * 4 + [both[1]] * 4, axis=0).T
        mean, inv = both[:, 0:1], both[:, 4:5]
        for a in range(0, height, TILE):
            e = a + TILE
            covar = total[0, a:e] / count - mean[a:e] * row_mean
            buf[a:e] = covar * covar * (inv[a:e] * row_inv)
            copy(a // TILE)

    def win_copy(t):
        return pltpu.make_async_copy(
            win_buf.at[pl.ds(t * TILE, TILE)], win_out.at[0, pl.ds(t * TILE, TILE)], sems.at[t])

    band_copy = pltpu.make_async_copy(
        band_buf.at[pl.ds(pl.multiple_of(off, 8), band)], band_out.at[0], sems.at[jw // TILE])
    squares(win_sum, j_stat, win_buf, jw, lambda t: win_copy(t).start())
    squares(band_sum, b_stat, band_buf, bw, lambda t: None)
    band_copy.start()
    for t in range(jw // TILE):
        win_copy(t).wait()
    band_copy.wait()


def shards(dosages):
    rows, width = dosages.shape
    shard_count = lax.axis_size("samp")
    windows = lax.axis_size("win")
    blocks = lax.axis_size("snp")
    jw = width * blocks // shard_count
    band = OV // shard_count
    bw = max(band, 128)
    bits = blocks.bit_length() - 1
    chunks = shard_count * PARTS
    part_rows = rows // PARTS
    sizes = (shard_count, windows, blocks, rows, width, jw, band, bw)
    dma = pltpu.SemaphoreType.DMA
    f32 = jnp.float32
    sums = (
        jax.ShapeDtypeStruct((1, jw, width), f32),
        jax.ShapeDtypeStruct((1, bw, width), f32),
        jax.ShapeDtypeStruct((2, 8, width), f32),
        jax.ShapeDtypeStruct((2, 8, jw), f32),
        jax.ShapeDtypeStruct((2, 8, bw), f32),
    )
    parts = pl.pallas_call(
        functools.partial(kernel, sizes),
        out_shape=sums,
        in_specs=[pl.BlockSpec(memory_space=pl.ANY)],
        out_specs=[pl.BlockSpec(memory_space=pltpu.VMEM)] * len(sums),
        scratch_shapes=[
            pltpu.VMEM((chunks, part_rows, width), jnp.bfloat16),
            pltpu.VMEM((chunks, part_rows, jw), jnp.bfloat16),
            pltpu.VMEM((chunks, part_rows, bw), jnp.bfloat16),
            dma((PARTS,)),
            dma((chunks,)), dma, dma, dma,
            dma((chunks,)), dma((bits,)),
            dma((chunks,)), dma((blocks - 1,)), dma,
        ],
        compiler_params=pltpu.CompilerParams(
            collective_id=0, has_side_effects=True, vmem_limit_bytes=24 * 2**20
        ),
    )(dosages)
    return pl.pallas_call(
        functools.partial(finish, sizes),
        out_shape=(
            jax.ShapeDtypeStruct((1, jw, width), f32),
            jax.ShapeDtypeStruct((1, band, width), f32),
        ),
        in_specs=[pl.BlockSpec(memory_space=pltpu.VMEM)] * len(sums),
        out_specs=[pl.BlockSpec(memory_space=pl.ANY)] * 2,
        scratch_shapes=[
            pltpu.VMEM((jw, width), f32),
            pltpu.VMEM((bw, width), f32),
            dma((jw // TILE + 1,)),
        ],
        compiler_params=pltpu.CompilerParams(vmem_limit_bytes=24 * 2**20),
    )(*parts)


def solution(mesh):
    return jax.shard_map(
        shards,
        mesh=mesh,
        in_specs=(P("samp", ("win", "snp")),),
        out_specs=(P("win", "samp", "snp"), P("win", "samp", "snp")),
        check_vma=False,
    )
```

```python
import functools
import heapq

import jax
import jax.numpy as jnp
from jax import lax
from jax.experimental import pallas as pl
from jax.experimental.pallas import tpu as pltpu
from jax.sharding import PartitionSpec as P

OV = 1024
VAR_FLOOR = 0.05
COLS = 2
PARTS = 4
LATE = PARTS // 2
PASS = 2
USE = 4
HEAD_START = 6000
TILE = 64
CLOSE = 4
END = 2
MESH = pl.DeviceIdType.MESH


def by_z(z, zz, c):
    return c >= LATE and abs(z - zz) == 1


def sends(line, z, item):
    side, zz, c = item
    out = []
    if side == 0:
        if zz <= z and z < line - 1:
            out.append((1, item))
        if zz >= z and z > 0:
            out.append((-1, item))
        if not by_z(z, zz, c):
            out.append((0, item))
        if c == PARTS - 1:
            for way, far in ((-1, line - 1), (1, 0)):
                if zz == far and 0 <= z + way < line and last_on(line, z, way):
                    out += [(way, (1, z, k)) for k in range(LATE, PARTS)]
    elif zz == z and c >= LATE:
        for way in (-1, 1):
            if 0 <= z + way < line and not last_on(line, z, way):
                out.append((way, item))
    return out


def last_on(line, z, way):
    return z < line // 2 if way < 0 else z >= line // 2


def plan(line):
    hop = 1.0
    lag = 0.35
    events = [(0.0, z * PARTS + c, z, (0, z, c)) for z in range(line) for c in range(PARTS)]
    heapq.heapify(events)
    free = {}
    order = [[] for _ in range(line)]
    count = line * PARTS
    while events:
        t, _, z, item = heapq.heappop(events)
        order[z].append(item)
        for way, (side, zz, c) in sends(line, z, item):
            begin = max(free.get((z, way), 0.0), t)
            free[z, way] = begin + hop
            moved = (side, zz, c) if way else (1 - side, zz, c)
            heapq.heappush(events, (begin + hop + lag, count, z + way, moved))
            count += 1
    for z in range(line // 2, line):
        order[z] = [(side, line - 1 - zz, c) for side, zz, c in order[line - 1 - z]]
    return order


def lookup(i, values):
    out = jnp.int32(0)
    for j, v in enumerate(values):
        if v:
            out = out + jnp.where(i == j, jnp.int32(v), jnp.int32(0))
    return out


def kernel(sizes, x_hbm, win_sum, band_sum, k_stat, j_stat, b_stat, k_buf, j_buf, b_buf,
           local_sem, k_recv, up_send, down_send, x_send, j_recv, j_send, b_recv, b_send, w_send):
    shard_count, windows, blocks, rows, width, jw, band, bw = sizes
    line = shard_count // COLS
    part_rows = rows // PARTS
    bits = blocks.bit_length() - 1
    chunks = shard_count * PARTS
    s = lax.axis_index("samp")
    n = lax.axis_index("snp")
    z = s // COLS
    x = s % COLS
    has_up = z < line - 1
    has_down = z > 0
    up = {"samp": jnp.minimum(s + COLS, shard_count - COLS + x)}
    down = {"samp": jnp.maximum(s - COLS, x)}
    across = {"samp": s + 1 - 2 * x}

    def bit(v, b):
        return (v // (1 << b)) % 2

    def flip(b):
        return {"snp": n + (1 << b) * (1 - 2 * bit(n, b))}

    def beside(delta):
        to = n
        for b in range(bits):
            if delta >> b & 1:
                to = to + (1 << b) * (1 - 2 * bit(n, b))
        return {"snp": to}

    j_home = (s * jw) // width
    j_off = pl.multiple_of((s * jw) % width, jw)
    b_home = (s * band) // width
    b_off = pl.multiple_of(((s * band) % width) // bw * bw, bw)
    j_rel = [(bit(n, b) + bit(j_home, b)) % 2 for b in range(bits)]

    def sends_on(rel, b):
        low = jnp.int32(0)
        for a in range(b + 1):
            low = low + rel[a]
        return low == 0

    def is_home(rel):
        total = jnp.int32(0)
        for r in rel:
            total = total + r
        return total == 0

    j_mine = is_home(j_rel)
    b_mine = n == b_home

    def k_copy(q, sem, to, src=None):
        return pltpu.make_async_remote_copy(
            src_ref=k_buf.at[q] if src is None else src, dst_ref=k_buf.at[q], send_sem=sem, recv_sem=k_recv.at[q],
            device_id=to, device_id_type=MESH)

    def slice_copy(src, buf, q, send, recv, to):
        return pltpu.make_async_remote_copy(
            src_ref=src, dst_ref=buf.at[q], send_sem=send, recv_sem=recv.at[q],
            device_id=to, device_id_type=MESH)

    order = plan(line)
    low = z < line // 2
    near_z = jnp.where(low, z, line - 1 - z)

    def item(o):
        code = jnp.int32(0)
        for half in range((line + 1) // 2):
            mine = lookup(o, [(side * line + zz) * PARTS + c for side, zz, c in order[half]])
            code = code + jnp.where(near_z == half, mine, 0)
        c = code % PARTS
        zz = (code // PARTS) % line
        side = code // (PARTS * line)
        zz = jnp.where(low, zz, line - 1 - zz)
        xx = jnp.where(side == 1, 1 - x, x)
        return side, zz, c, (zz * COLS + xx) * PARTS + c

    def skips_x(zz, c):
        return (c >= LATE) & ((zz == z + 1) | (zz == z - 1))

    crossed = [(s + 1 - 2 * x) * PARTS + c for c in range(LATE, PARTS)]
    up_last = has_up & (z >= line // 2)
    down_last = has_down & (z < line // 2)
    up_soon = has_up & (z < line // 2)
    down_soon = has_down & (z >= line // 2)

    for c in range(PARTS):
        pltpu.make_async_copy(x_hbm.at[pl.ds(c * part_rows, part_rows)],
                              k_buf.at[s * PARTS + c], local_sem.at[c]).start()

    barrier = pltpu.get_barrier_semaphore()

    def greet(to):
        pl.semaphore_signal(barrier, inc=1, device_id=to, device_id_type=MESH)

    pl.when(has_up)(lambda: greet(up))
    pl.when(has_down)(lambda: greet(down))
    greet(across)
    for delta in range(1, blocks):
        greet(beside(delta))
    expected = blocks
    if windows > 1:
        w = lax.axis_index("win")
        before = {"win": (w + windows - 1) % windows}
        after = {"win": (w + 1) % windows}
        greet(before)
        greet(after)
        expected += 2
    pl.semaphore_wait(barrier, expected + has_up.astype(jnp.int32) + has_down.astype(jnp.int32))

    pl.when((n > 0) & (n < blocks - 1))(lambda: pl.delay(HEAD_START))

    k_stat[...] = jnp.zeros_like(k_stat)
    j_stat[...] = jnp.zeros_like(j_stat)
    b_stat[...] = jnp.zeros_like(b_stat)
    win_sum[...] = jnp.zeros_like(win_sum)
    band_sum[...] = jnp.zeros_like(band_sum)

    def take(side, zz, c, q):
        mine = (side == 0) & (zz == z)

        @pl.when(mine)
        def _():
            own = x_hbm.at[pl.ds(c * part_rows, part_rows)]
            pl.when(has_up)(lambda: k_copy(q, up_send, up, own).start())
            pl.when(has_down)(lambda: k_copy(q, down_send, down, own).start())
            k_copy(q, x_send, across, own).start()
            pltpu.make_async_copy(own, k_buf.at[q], local_sem.at[c]).wait()

        @pl.when(jnp.logical_not(mine))
        def _():
            k_copy(q, x_send, across).wait_recv()

        @pl.when((side == 0) & (zz < z) & has_up)
        def _():
            k_copy(q, up_send, up).start()

        @pl.when((side == 0) & (zz > z) & has_down)
        def _():
            k_copy(q, down_send, down).start()

        @pl.when((side == 0) & (zz != z) & jnp.logical_not(skips_x(zz, c)))
        def _():
            k_copy(q, x_send, across).start()

        if line > 1:
            passes = (side == 1) & (zz == z) & (c >= LATE)
            ends = (side == 0) & (c == PARTS - 1)

            @pl.when(passes & up_soon)
            def _():
                k_copy(q, up_send, up).start()

            @pl.when(passes & down_soon)
            def _():
                k_copy(q, down_send, down).start()

            @pl.when(ends & (zz == 0) & up_last)
            def _():
                for k in crossed:
                    k_copy(k, up_send, up).start()

            @pl.when(ends & (zz == line - 1) & down_last)
            def _():
                for k in crossed:
                    k_copy(k, down_send, down).start()

        for b in reversed(range(bits)):
            @pl.when(j_mine)
            def _():
                slice_copy(k_buf.at[q, :, pl.ds(j_off, jw)], j_buf, q, j_send.at[b], j_recv, flip(b)).start()

        if windows == 1:
            @pl.when(b_mine)
            def _():
                for delta in reversed(range(1, blocks)):
                    slice_copy(k_buf.at[q, :, pl.ds(b_off, bw)], b_buf, q, b_send.at[delta - 1], b_recv,
                               beside(delta)).start()
        if windows > 1:
            @pl.when(b_mine)
            def _():
                slice_copy(k_buf.at[q, :, pl.ds(b_off, bw)], b_buf, q, w_send, b_recv, before).start()

    def j_arrive(q):
        slice_copy(k_buf.at[q, :, pl.ds(j_off, jw)], j_buf, q, j_send.at[0], j_recv, flip(0)).wait_recv()

    def b_arrive(q):
        slice_copy(k_buf.at[q, :, pl.ds(b_off, bw)], b_buf, q, b_send.at[0], b_recv, flip(0)).wait_recv()

    j_passes = (j_rel[0] == 0) & jnp.logical_not(j_mine)

    def forward(q):
        @pl.when(j_passes)
        def _():
            j_arrive(q)
            for b in reversed(range(bits)):
                @pl.when(sends_on(j_rel, b))
                def _():
                    slice_copy(j_buf.at[q], j_buf, q, j_send.at[b], j_recv, flip(b)).start()

        if windows > 1:
            @pl.when(b_mine)
            def _():
                b_arrive(q)
                for delta in reversed(range(1, blocks)):
                    slice_copy(b_buf.at[q], b_buf, q, b_send.at[delta - 1], b_recv, beside(delta)).start()

    def add_stats(stat, block):
        wide = block.astype(jnp.float32).reshape(block.shape[0] // 8, 8, block.shape[-1])
        stat[0] += jnp.sum(wide, axis=0)
        stat[1] += jnp.sum(wide * wide, axis=0)

    def pair(a, b):
        return lax.dot_general(a, b, (((0,), (0,)), ((), ())), preferred_element_type=jnp.float32)

    def arrive(q):
        @pl.when(j_rel[0] != 0)
        def _():
            j_arrive(q)

        @pl.when(j_mine)
        def _():
            j_buf[q] = k_buf[q, :, pl.ds(j_off, jw)]

        @pl.when(jnp.logical_not(b_mine))
        def _():
            b_arrive(q)

        if windows == 1:
            @pl.when(b_mine)
            def _():
                b_buf[q] = k_buf[q, :, pl.ds(b_off, bw)]

    def compute(*places):
        for q in places:
            arrive(q)
        whole, j_cols, b_cols = (
            jnp.concatenate([buf[q] for q in places], axis=0) for buf in (k_buf, j_buf, b_buf))
        add_stats(k_stat, whole)
        add_stats(j_stat, j_cols)
        add_stats(b_stat, b_cols)
        win_sum[0] += pair(j_cols, whole)
        band_sum[0] += pair(b_cols, whole)

    def place(o):
        return item(o)[3]

    def each(first, last, what):
        def one(i, _):
            what(place(i))

        lax.fori_loop(first, last, one, None)

    def two(i, _):
        compute(place(2 * i), place(2 * i + 1))

    def add_up(first, last):
        lax.fori_loop(first // 2, last // 2, two, None)

    def summed(o):
        return jnp.maximum(0, o + 1 - USE)

    def step(o, held):
        side, zz, c, q = item(o)
        take(side, zz, c, q)

        @pl.when(o >= PASS)
        def _():
            forward(held[PASS - 1])

        add_up(summed(o - 1), summed(o))
        return (q, *held[:-1])

    at_end = (z == 0) | (z == line - 1)
    eager = at_end & (j_home == b_home)
    closing = chunks - CLOSE
    lax.fori_loop(0, closing, step, (jnp.int32(0),) * PASS)

    def passed(o):
        return jnp.where(o < closing, closing - PASS, jnp.where(eager, o, o - 1))

    def summed_in(o):
        lag = jnp.where(eager, 0, jnp.where(at_end, END, USE))
        last = jnp.where(eager, chunks - 2, chunks - 4)
        return jnp.where(o < closing, closing - USE, jnp.where(o == chunks - 1, last, o - lag))

    def close(o, _):
        each(passed(o - 1), passed(o), forward)
        add_up(summed_in(o - 1), summed_in(o))
        take(*item(o))

    lax.fori_loop(closing, chunks, close, None)
    each(passed(chunks - 1), chunks - 1, forward)
    add_up(summed_in(chunks - 1), chunks - 2)

    def sent(buf, number, sem):
        part = buf.at[pl.ds(0, number)]
        pltpu.make_async_remote_copy(
            src_ref=part, dst_ref=part, send_sem=sem, recv_sem=k_recv.at[0],
            device_id=across, device_id_type=MESH).wait_send()

    for zz in range(line):
        over = sum(not by_z(zz, a, c) for a in range(line) for c in range(PARTS))

        @pl.when(z == zz)
        def _():
            if zz < line - 1:
                sent(k_buf, (zz + 1) * PARTS + PARTS - LATE, up_send)
            if zz > 0:
                sent(k_buf, (line - zz) * PARTS + PARTS - LATE, down_send)
            sent(k_buf, over, x_send)

    each(chunks - 1, chunks, forward)
    add_up(chunks - 2, chunks)

    for b in range(bits):
        @pl.when(sends_on(j_rel, b))
        def _():
            sent(j_buf, chunks, j_send.at[b])

    @pl.when(b_mine)
    def _():
        for delta in range(1, blocks):
            sent(b_buf, chunks, b_send.at[delta - 1])
        if windows > 1:
            sent(b_buf, chunks, w_send)


def finish(sizes, win_sum, band_sum, k_stat, j_stat, b_stat, win_out, band_out, win_buf, band_buf, sems):
    shard_count, windows, blocks, rows, width, jw, band, bw = sizes
    count = jnp.float32(rows * shard_count)
    off = (lax.axis_index("samp") * band) % bw

    def moments(total, square):
        mean = total / count
        return mean, 1.0 / jnp.maximum(square / count - mean * mean, VAR_FLOOR)

    row_mean, row_inv = moments(jnp.sum(k_stat[0], axis=0, keepdims=True), jnp.sum(k_stat[1], axis=0, keepdims=True))

    def squares(total, stat, buf, height, copy):
        both = moments(jnp.sum(stat[0], axis=0, keepdims=True), jnp.sum(stat[1], axis=0, keepdims=True))
        both = jnp.concatenate([both[0]] * 4 + [both[1]] * 4, axis=0).T
        mean, inv = both[:, 0:1], both[:, 4:5]
        for a in range(0, height, TILE):
            e = a + TILE
            covar = total[0, a:e] / count - mean[a:e] * row_mean
            buf[a:e] = covar * covar * (inv[a:e] * row_inv)
            copy(a // TILE)

    def win_copy(t):
        return pltpu.make_async_copy(
            win_buf.at[pl.ds(t * TILE, TILE)], win_out.at[0, pl.ds(t * TILE, TILE)], sems.at[t])

    band_copy = pltpu.make_async_copy(
        band_buf.at[pl.ds(pl.multiple_of(off, 8), band)], band_out.at[0], sems.at[jw // TILE])
    squares(win_sum, j_stat, win_buf, jw, lambda t: win_copy(t).start())
    squares(band_sum, b_stat, band_buf, bw, lambda t: None)
    band_copy.start()
    for t in range(jw // TILE):
        win_copy(t).wait()
    band_copy.wait()


def shards(dosages):
    rows, width = dosages.shape
    shard_count = lax.axis_size("samp")
    windows = lax.axis_size("win")
    blocks = lax.axis_size("snp")
    jw = width * blocks // shard_count
    band = OV // shard_count
    bw = max(band, 128)
    bits = blocks.bit_length() - 1
    chunks = shard_count * PARTS
    part_rows = rows // PARTS
    sizes = (shard_count, windows, blocks, rows, width, jw, band, bw)
    dma = pltpu.SemaphoreType.DMA
    f32 = jnp.float32
    sums = (
        jax.ShapeDtypeStruct((1, jw, width), f32),
        jax.ShapeDtypeStruct((1, bw, width), f32),
        jax.ShapeDtypeStruct((2, 8, width), f32),
        jax.ShapeDtypeStruct((2, 8, jw), f32),
        jax.ShapeDtypeStruct((2, 8, bw), f32),
    )
    parts = pl.pallas_call(
        functools.partial(kernel, sizes),
        out_shape=sums,
        in_specs=[pl.BlockSpec(memory_space=pl.ANY)],
        out_specs=[pl.BlockSpec(memory_space=pltpu.VMEM)] * len(sums),
        scratch_shapes=[
            pltpu.VMEM((chunks, part_rows, width), jnp.bfloat16),
            pltpu.VMEM((chunks, part_rows, jw), jnp.bfloat16),
            pltpu.VMEM((chunks, part_rows, bw), jnp.bfloat16),
            dma((PARTS,)),
            dma((chunks,)), dma, dma, dma,
            dma((chunks,)), dma((bits,)),
            dma((chunks,)), dma((blocks - 1,)), dma,
        ],
        compiler_params=pltpu.CompilerParams(
            collective_id=0, has_side_effects=True, vmem_limit_bytes=24 * 2**20
        ),
    )(dosages)
    return pl.pallas_call(
        functools.partial(finish, sizes),
        out_shape=(
            jax.ShapeDtypeStruct((1, jw, width), f32),
            jax.ShapeDtypeStruct((1, band, width), f32),
        ),
        in_specs=[pl.BlockSpec(memory_space=pltpu.VMEM)] * len(sums),
        out_specs=[pl.BlockSpec(memory_space=pl.ANY)] * 2,
        scratch_shapes=[
            pltpu.VMEM((jw, width), f32),
            pltpu.VMEM((bw, width), f32),
            dma((jw // TILE + 1,)),
        ],
        compiler_params=pltpu.CompilerParams(vmem_limit_bytes=24 * 2**20),
    )(*parts)


def solution(mesh):
    return jax.shard_map(
        shards,
        mesh=mesh,
        in_specs=(P("samp", ("win", "snp")),),
        out_specs=(P("win", "samp", "snp"), P("win", "samp", "snp")),
        check_vma=False,
    )
```

```python
import functools
import heapq

import jax
import jax.numpy as jnp
from jax import lax
from jax.experimental import pallas as pl
from jax.experimental.pallas import tpu as pltpu
from jax.sharding import PartitionSpec as P

OV = 1024
VAR_FLOOR = 0.05
COLS = 2
PARTS = 4
LATE = PARTS // 2
PASS = 2
USE = 4
HEAD_START = 5700
TILE = 64
CLOSE = 4
END = 2
MESH = pl.DeviceIdType.MESH


def by_z(z, zz, c):
    return c >= LATE and abs(z - zz) == 1


def sends(line, z, item):
    side, zz, c = item
    out = []
    if side == 0:
        if zz <= z and z < line - 1:
            out.append((1, item))
        if zz >= z and z > 0:
            out.append((-1, item))
        if not by_z(z, zz, c):
            out.append((0, item))
        if c == PARTS - 1:
            for way, far in ((-1, line - 1), (1, 0)):
                if zz == far and 0 <= z + way < line and last_on(line, z, way):
                    out += [(way, (1, z, k)) for k in range(LATE, PARTS)]
    elif zz == z and c >= LATE:
        for way in (-1, 1):
            if 0 <= z + way < line and not last_on(line, z, way):
                out.append((way, item))
    return out


def last_on(line, z, way):
    return z < line // 2 if way < 0 else z >= line // 2


def plan(line):
    hop = 1.0
    lag = 0.35
    events = [(0.0, z * PARTS + c, z, (0, z, c)) for z in range(line) for c in range(PARTS)]
    heapq.heapify(events)
    free = {}
    order = [[] for _ in range(line)]
    count = line * PARTS
    while events:
        t, _, z, item = heapq.heappop(events)
        order[z].append(item)
        for way, (side, zz, c) in sends(line, z, item):
            begin = max(free.get((z, way), 0.0), t)
            free[z, way] = begin + hop
            moved = (side, zz, c) if way else (1 - side, zz, c)
            heapq.heappush(events, (begin + hop + lag, count, z + way, moved))
            count += 1
    for z in range(line // 2, line):
        order[z] = [(side, line - 1 - zz, c) for side, zz, c in order[line - 1 - z]]
    return order


def lookup(i, values):
    out = jnp.int32(0)
    for j, v in enumerate(values):
        if v:
            out = out + jnp.where(i == j, jnp.int32(v), jnp.int32(0))
    return out


def kernel(sizes, x_hbm, win_sum, band_sum, k_stat, j_stat, b_stat, k_buf, j_buf, b_buf,
           local_sem, k_recv, up_send, down_send, x_send, j_recv, j_send, b_recv, b_send, w_send):
    shard_count, windows, blocks, rows, width, jw, band, bw = sizes
    line = shard_count // COLS
    part_rows = rows // PARTS
    bits = blocks.bit_length() - 1
    chunks = shard_count * PARTS
    s = lax.axis_index("samp")
    n = lax.axis_index("snp")
    z = s // COLS
    x = s % COLS
    has_up = z < line - 1
    has_down = z > 0
    up = {"samp": jnp.minimum(s + COLS, shard_count - COLS + x)}
    down = {"samp": jnp.maximum(s - COLS, x)}
    across = {"samp": s + 1 - 2 * x}

    def bit(v, b):
        return (v // (1 << b)) % 2

    def flip(b):
        return {"snp": n + (1 << b) * (1 - 2 * bit(n, b))}

    def beside(delta):
        to = n
        for b in range(bits):
            if delta >> b & 1:
                to = to + (1 << b) * (1 - 2 * bit(n, b))
        return {"snp": to}

    j_home = (s * jw) // width
    j_off = pl.multiple_of((s * jw) % width, jw)
    b_home = (s * band) // width
    b_off = pl.multiple_of(((s * band) % width) // bw * bw, bw)
    j_rel = [(bit(n, b) + bit(j_home, b)) % 2 for b in range(bits)]

    def sends_on(rel, b):
        low = jnp.int32(0)
        for a in range(b + 1):
            low = low + rel[a]
        return low == 0

    def is_home(rel):
        total = jnp.int32(0)
        for r in rel:
            total = total + r
        return total == 0

    j_mine = is_home(j_rel)
    b_mine = n == b_home

    def k_copy(q, sem, to, src=None):
        return pltpu.make_async_remote_copy(
            src_ref=k_buf.at[q] if src is None else src, dst_ref=k_buf.at[q], send_sem=sem, recv_sem=k_recv.at[q],
            device_id=to, device_id_type=MESH)

    def slice_copy(src, buf, q, send, recv, to):
        return pltpu.make_async_remote_copy(
            src_ref=src, dst_ref=buf.at[q], send_sem=send, recv_sem=recv.at[q],
            device_id=to, device_id_type=MESH)

    order = plan(line)
    low = z < line // 2
    near_z = jnp.where(low, z, line - 1 - z)

    def item(o):
        code = jnp.int32(0)
        for half in range((line + 1) // 2):
            mine = lookup(o, [(side * line + zz) * PARTS + c for side, zz, c in order[half]])
            code = code + jnp.where(near_z == half, mine, 0)
        c = code % PARTS
        zz = (code // PARTS) % line
        side = code // (PARTS * line)
        zz = jnp.where(low, zz, line - 1 - zz)
        xx = jnp.where(side == 1, 1 - x, x)
        return side, zz, c, (zz * COLS + xx) * PARTS + c

    def skips_x(zz, c):
        return (c >= LATE) & ((zz == z + 1) | (zz == z - 1))

    crossed = [(s + 1 - 2 * x) * PARTS + c for c in range(LATE, PARTS)]
    up_last = has_up & (z >= line // 2)
    down_last = has_down & (z < line // 2)
    up_soon = has_up & (z < line // 2)
    down_soon = has_down & (z >= line // 2)

    for c in range(PARTS):
        pltpu.make_async_copy(x_hbm.at[pl.ds(c * part_rows, part_rows)],
                              k_buf.at[s * PARTS + c], local_sem.at[c]).start()

    barrier = pltpu.get_barrier_semaphore()

    def greet(to):
        pl.semaphore_signal(barrier, inc=1, device_id=to, device_id_type=MESH)

    pl.when(has_up)(lambda: greet(up))
    pl.when(has_down)(lambda: greet(down))
    greet(across)
    for delta in range(1, blocks):
        greet(beside(delta))
    expected = blocks
    if windows > 1:
        w = lax.axis_index("win")
        before = {"win": (w + windows - 1) % windows}
        after = {"win": (w + 1) % windows}
        greet(before)
        greet(after)
        expected += 2
    pl.semaphore_wait(barrier, expected + has_up.astype(jnp.int32) + has_down.astype(jnp.int32))

    pl.when((n > 0) & (n < blocks - 1))(lambda: pl.delay(HEAD_START))

    k_stat[...] = jnp.zeros_like(k_stat)
    j_stat[...] = jnp.zeros_like(j_stat)
    b_stat[...] = jnp.zeros_like(b_stat)
    win_sum[...] = jnp.zeros_like(win_sum)
    band_sum[...] = jnp.zeros_like(band_sum)

    def take(side, zz, c, q):
        mine = (side == 0) & (zz == z)

        @pl.when(mine)
        def _():
            own = x_hbm.at[pl.ds(c * part_rows, part_rows)]
            pl.when(has_up)(lambda: k_copy(q, up_send, up, own).start())
            pl.when(has_down)(lambda: k_copy(q, down_send, down, own).start())
            k_copy(q, x_send, across, own).start()
            pltpu.make_async_copy(own, k_buf.at[q], local_sem.at[c]).wait()

        @pl.when(jnp.logical_not(mine))
        def _():
            k_copy(q, x_send, across).wait_recv()

        @pl.when((side == 0) & (zz < z) & has_up)
        def _():
            k_copy(q, up_send, up).start()

        @pl.when((side == 0) & (zz > z) & has_down)
        def _():
            k_copy(q, down_send, down).start()

        @pl.when((side == 0) & (zz != z) & jnp.logical_not(skips_x(zz, c)))
        def _():
            k_copy(q, x_send, across).start()

        if line > 1:
            passes = (side == 1) & (zz == z) & (c >= LATE)
            ends = (side == 0) & (c == PARTS - 1)

            @pl.when(passes & up_soon)
            def _():
                k_copy(q, up_send, up).start()

            @pl.when(passes & down_soon)
            def _():
                k_copy(q, down_send, down).start()

            @pl.when(ends & (zz == 0) & up_last)
            def _():
                for k in crossed:
                    k_copy(k, up_send, up).start()

            @pl.when(ends & (zz == line - 1) & down_last)
            def _():
                for k in crossed:
                    k_copy(k, down_send, down).start()

        for b in reversed(range(bits)):
            @pl.when(j_mine)
            def _():
                slice_copy(k_buf.at[q, :, pl.ds(j_off, jw)], j_buf, q, j_send.at[b], j_recv, flip(b)).start()

        if windows == 1:
            @pl.when(b_mine)
            def _():
                for delta in reversed(range(1, blocks)):
                    slice_copy(k_buf.at[q, :, pl.ds(b_off, bw)], b_buf, q, b_send.at[delta - 1], b_recv,
                               beside(delta)).start()
        if windows > 1:
            @pl.when(b_mine)
            def _():
                slice_copy(k_buf.at[q, :, pl.ds(b_off, bw)], b_buf, q, w_send, b_recv, before).start()

    def j_arrive(q):
        slice_copy(k_buf.at[q, :, pl.ds(j_off, jw)], j_buf, q, j_send.at[0], j_recv, flip(0)).wait_recv()

    def b_arrive(q):
        slice_copy(k_buf.at[q, :, pl.ds(b_off, bw)], b_buf, q, b_send.at[0], b_recv, flip(0)).wait_recv()

    j_passes = (j_rel[0] == 0) & jnp.logical_not(j_mine)

    def forward(q):
        @pl.when(j_passes)
        def _():
            j_arrive(q)
            for b in reversed(range(bits)):
                @pl.when(sends_on(j_rel, b))
                def _():
                    slice_copy(j_buf.at[q], j_buf, q, j_send.at[b], j_recv, flip(b)).start()

        if windows > 1:
            @pl.when(b_mine)
            def _():
                b_arrive(q)
                for delta in reversed(range(1, blocks)):
                    slice_copy(b_buf.at[q], b_buf, q, b_send.at[delta - 1], b_recv, beside(delta)).start()

    def add_stats(stat, block):
        wide = block.astype(jnp.float32).reshape(block.shape[0] // 8, 8, block.shape[-1])
        stat[0] += jnp.sum(wide, axis=0)
        stat[1] += jnp.sum(wide * wide, axis=0)

    def pair(a, b):
        return lax.dot_general(a, b, (((0,), (0,)), ((), ())), preferred_element_type=jnp.float32)

    def arrive(q):
        @pl.when(j_rel[0] != 0)
        def _():
            j_arrive(q)

        @pl.when(j_mine)
        def _():
            j_buf[q] = k_buf[q, :, pl.ds(j_off, jw)]

        @pl.when(jnp.logical_not(b_mine))
        def _():
            b_arrive(q)

        if windows == 1:
            @pl.when(b_mine)
            def _():
                b_buf[q] = k_buf[q, :, pl.ds(b_off, bw)]

    def compute(*places):
        for q in places:
            arrive(q)
        whole, j_cols, b_cols = (
            jnp.concatenate([buf[q] for q in places], axis=0) for buf in (k_buf, j_buf, b_buf))
        add_stats(k_stat, whole)
        add_stats(j_stat, j_cols)
        add_stats(b_stat, b_cols)
        win_sum[0] += pair(j_cols, whole)
        band_sum[0] += pair(b_cols, whole)

    def place(o):
        return item(o)[3]

    def each(first, last, what):
        def one(i, _):
            what(place(i))

        lax.fori_loop(first, last, one, None)

    def two(i, _):
        compute(place(2 * i), place(2 * i + 1))

    def add_up(first, last):
        lax.fori_loop(first // 2, last // 2, two, None)

    def summed(o):
        return jnp.maximum(0, o + 1 - USE)

    def step(o, held):
        side, zz, c, q = item(o)
        take(side, zz, c, q)

        @pl.when(o >= PASS)
        def _():
            forward(held[PASS - 1])

        add_up(summed(o - 1), summed(o))
        return (q, *held[:-1])

    at_end = (z == 0) | (z == line - 1)
    eager = at_end & (j_home == b_home)
    closing = chunks - CLOSE
    lax.fori_loop(0, closing, step, (jnp.int32(0),) * PASS)

    def passed(o):
        return jnp.where(o < closing, closing - PASS, jnp.where(eager, o, o - 1))

    def summed_in(o):
        lag = jnp.where(eager, 0, jnp.where(at_end, END, USE))
        last = jnp.where(eager, chunks - 2, chunks - 4)
        return jnp.where(o < closing, closing - USE, jnp.where(o == chunks - 1, last, o - lag))

    def close(o, _):
        each(passed(o - 1), passed(o), forward)
        add_up(summed_in(o - 1), summed_in(o))
        take(*item(o))

    lax.fori_loop(closing, chunks, close, None)
    each(passed(chunks - 1), chunks - 1, forward)
    add_up(summed_in(chunks - 1), chunks - 2)

    def sent(buf, number, sem):
        part = buf.at[pl.ds(0, number)]
        pltpu.make_async_remote_copy(
            src_ref=part, dst_ref=part, send_sem=sem, recv_sem=k_recv.at[0],
            device_id=across, device_id_type=MESH).wait_send()

    for zz in range(line):
        over = sum(not by_z(zz, a, c) for a in range(line) for c in range(PARTS))

        @pl.when(z == zz)
        def _():
            if zz < line - 1:
                sent(k_buf, (zz + 1) * PARTS + PARTS - LATE, up_send)
            if zz > 0:
                sent(k_buf, (line - zz) * PARTS + PARTS - LATE, down_send)
            sent(k_buf, over, x_send)

    each(chunks - 1, chunks, forward)
    add_up(chunks - 2, chunks)

    for b in range(bits):
        @pl.when(sends_on(j_rel, b))
        def _():
            sent(j_buf, chunks, j_send.at[b])

    @pl.when(b_mine)
    def _():
        for delta in range(1, blocks):
            sent(b_buf, chunks, b_send.at[delta - 1])
        if windows > 1:
            sent(b_buf, chunks, w_send)


def finish(sizes, win_sum, band_sum, k_stat, j_stat, b_stat, win_out, band_out, win_buf, band_buf, sems):
    shard_count, windows, blocks, rows, width, jw, band, bw = sizes
    count = jnp.float32(rows * shard_count)
    off = (lax.axis_index("samp") * band) % bw

    def moments(total, square):
        mean = total / count
        return mean, 1.0 / jnp.maximum(square / count - mean * mean, VAR_FLOOR)

    row_mean, row_inv = moments(jnp.sum(k_stat[0], axis=0, keepdims=True), jnp.sum(k_stat[1], axis=0, keepdims=True))

    def squares(total, stat, buf, height, copy):
        both = moments(jnp.sum(stat[0], axis=0, keepdims=True), jnp.sum(stat[1], axis=0, keepdims=True))
        both = jnp.concatenate([both[0]] * 4 + [both[1]] * 4, axis=0).T
        mean, inv = both[:, 0:1], both[:, 4:5]
        for a in range(0, height, TILE):
            e = a + TILE
            covar = total[0, a:e] / count - mean[a:e] * row_mean
            buf[a:e] = covar * covar * (inv[a:e] * row_inv)
            copy(a // TILE)

    def win_copy(t):
        return pltpu.make_async_copy(
            win_buf.at[pl.ds(t * TILE, TILE)], win_out.at[0, pl.ds(t * TILE, TILE)], sems.at[t])

    band_copy = pltpu.make_async_copy(
        band_buf.at[pl.ds(pl.multiple_of(off, 8), band)], band_out.at[0], sems.at[jw // TILE])
    squares(win_sum, j_stat, win_buf, jw, lambda t: win_copy(t).start())
    squares(band_sum, b_stat, band_buf, bw, lambda t: None)
    band_copy.start()
    for t in range(jw // TILE):
        win_copy(t).wait()
    band_copy.wait()


def shards(dosages):
    rows, width = dosages.shape
    shard_count = lax.axis_size("samp")
    windows = lax.axis_size("win")
    blocks = lax.axis_size("snp")
    jw = width * blocks // shard_count
    band = OV // shard_count
    bw = max(band, 128)
    bits = blocks.bit_length() - 1
    chunks = shard_count * PARTS
    part_rows = rows // PARTS
    sizes = (shard_count, windows, blocks, rows, width, jw, band, bw)
    dma = pltpu.SemaphoreType.DMA
    f32 = jnp.float32
    sums = (
        jax.ShapeDtypeStruct((1, jw, width), f32),
        jax.ShapeDtypeStruct((1, bw, width), f32),
        jax.ShapeDtypeStruct((2, 8, width), f32),
        jax.ShapeDtypeStruct((2, 8, jw), f32),
        jax.ShapeDtypeStruct((2, 8, bw), f32),
    )
    parts = pl.pallas_call(
        functools.partial(kernel, sizes),
        out_shape=sums,
        in_specs=[pl.BlockSpec(memory_space=pl.ANY)],
        out_specs=[pl.BlockSpec(memory_space=pltpu.VMEM)] * len(sums),
        scratch_shapes=[
            pltpu.VMEM((chunks, part_rows, width), jnp.bfloat16),
            pltpu.VMEM((chunks, part_rows, jw), jnp.bfloat16),
            pltpu.VMEM((chunks, part_rows, bw), jnp.bfloat16),
            dma((PARTS,)),
            dma((chunks,)), dma, dma, dma,
            dma((chunks,)), dma((bits,)),
            dma((chunks,)), dma((blocks - 1,)), dma,
        ],
        compiler_params=pltpu.CompilerParams(
            collective_id=0, has_side_effects=True, vmem_limit_bytes=24 * 2**20
        ),
    )(dosages)
    return pl.pallas_call(
        functools.partial(finish, sizes),
        out_shape=(
            jax.ShapeDtypeStruct((1, jw, width), f32),
            jax.ShapeDtypeStruct((1, band, width), f32),
        ),
        in_specs=[pl.BlockSpec(memory_space=pltpu.VMEM)] * len(sums),
        out_specs=[pl.BlockSpec(memory_space=pl.ANY)] * 2,
        scratch_shapes=[
            pltpu.VMEM((jw, width), f32),
            pltpu.VMEM((bw, width), f32),
            dma((jw // TILE + 1,)),
        ],
        compiler_params=pltpu.CompilerParams(vmem_limit_bytes=24 * 2**20),
    )(*parts)


def solution(mesh):
    return jax.shard_map(
        shards,
        mesh=mesh,
        in_specs=(P("samp", ("win", "snp")),),
        out_specs=(P("win", "samp", "snp"), P("win", "samp", "snp")),
        check_vma=False,
    )
```
